32 devices in a mesh: head: 8 (over y, x, core), level: 4 (over z).
Axes of the slice: x: 2, y: 2, z: 4, core: 2. Of those that a mesh axis runs over, the one named last changes fastest.
Arguments:
- features: float32 [64, 4096], P(None, ('head', 'level')), may hold values from -6 to 6
- in_gain: float32 [4096], replicated, may hold values from 0.25 to 1.75
- in_weight: bfloat16 [4096, 4288], P(None, 'head'), may hold values from -0.09375 to 0.09375
- level_bias: float32 [8, 24], P('head'), may hold values from -4 to 252
- states: bfloat16 [64, 8, 24, 128, 128], P(None, 'head', 'level'), may hold values from -1.25 to 1.25
- positions: int32 [64], replicated, may hold values from 1 to 262143
- out_gain: float32 [1024], P('head'), may hold values from 0.25 to 1.75
- out_weight: bfloat16 [1024, 4096], P('head', 'level'), may hold values from -0.1875 to 0.1875
Outputs:
- output: float32 [64, 4096], P('head', 'level')
The draws below stay inside these ranges and needn't reach their ends.
Inputs may be any that keep to these rules, and one draw needn't show every extreme that they name: `positions`: positions below 2 ** 18, so levels from 19 on are never occupied.
All inputs are finite; a program needn't handle non-finite values.
Results may differ from the reference program's by a relative error of at most 0.0066.
Values sent between devices are 32-bit elements; how exact they have to be, the bound alone decides.
A program may use at most 64 MiB of HBM per device.

```python
import jax
import jax.numpy as jnp
from jax import lax

WIDTH = 4096
HEADS = 8
KEY_DIM = 128
VAL_DIM = 128
LEVELS = 24
PROJ = 536
SEQS = 64


def draw_level_bias(key, part):
    first = jax.random.fold_in(jax.random.fold_in(key, 7), 0)
    return jnp.clip(jax.random.normal(first, (HEADS, LEVELS), jnp.float32), -4.0, 4.0)


def plant(result, stream_key, smallest, top_value):
    place = [jax.random.randint(jax.random.fold_in(stream_key, axis), (), 0, length) for axis, length in enumerate(result.shape)]
    widest = result.shape.index(max(result.shape))
    neighbour = place[:widest] + [(place[widest] + 1) % result.shape[widest]] + place[widest + 1:]
    return result.at[tuple(place)].set(smallest).at[tuple(neighbour)].set(top_value)


def steps_of(rng, shape, cuts, low, high):
    level, own = 1.0, jax.random.fold_in(rng, 6)
    for axis_at, parts in cuts:
        heights = jnp.exp(jax.random.uniform(jax.random.fold_in(own, axis_at), (parts,), jnp.float32, low / len(cuts), high / len(cuts)))
        level = level * jnp.repeat(heights, shape[axis_at] // parts).reshape([-1 if axis == axis_at else 1 for axis in range(len(shape))])
    return level


def noise(stream_key, shape, spread, most, cuts=(), kind=jnp.bfloat16):
    level = steps_of(stream_key, shape, cuts, -0.22, 0.18) if cuts else 1.0
    array = jax.random.normal(stream_key, shape, jnp.float32) * spread * level
    return jnp.minimum(jnp.maximum(array, -most), most).astype(kind)


def setup_inputs(seed: int = 0) -> dict:
    arg_keys = jax.random.split(jax.random.key(seed), 9)
    return {
        "features": noise(arg_keys[0], (SEQS, WIDTH), 1.0, 6.0, ((1, 32),), jnp.float32),
        "in_gain": jnp.clip(1.0 + 0.15 * jax.random.normal(arg_keys[1], (WIDTH,), jnp.float32), 0.25, 1.75),
        "in_weight": noise(arg_keys[2], (WIDTH, HEADS * PROJ), WIDTH ** -0.5, 0.09375, ((1, 8),)),
        "level_bias": draw_level_bias(jax.random.fold_in(arg_keys[8], 71), 0),
        "states": noise(arg_keys[4], (SEQS, HEADS, LEVELS, KEY_DIM, VAL_DIM), (KEY_DIM ** -0.5), 1.25, ((1, 8), (2, 4))),
        "positions": plant(jax.random.randint(arg_keys[5], (SEQS,), 1, 262144), jax.random.fold_in(arg_keys[5], 1), 1, 262143).astype(jnp.int32),
        "out_gain": jnp.clip(1.0 + 0.15 * jax.random.normal(arg_keys[6], (HEADS * VAL_DIM,), jnp.float32), 0.25, 1.75),
        "out_weight": noise(arg_keys[7], (HEADS * VAL_DIM, WIDTH), (HEADS * VAL_DIM) ** -0.5, 0.1875, ((0, 8), (1, 4))),
    }


def occupancy(positions, level_ids):
    shifted = jnp.right_shift(positions[:, None], jnp.maximum(level_ids - 1, 0)[None, :])
    bits = jnp.bitwise_and(shifted, 1).astype(jnp.int32)
    first = (level_ids[None, :] == 0).astype(jnp.int32)
    return jnp.maximum(first, bits)[:, None, :]

def reference(features, in_gain, in_weight, level_bias, states, positions, out_gain, out_weight):
    squares = lax.optimization_barrier(jnp.sum(features * features, axis=1))
    row_scale = lax.rsqrt(squares / WIDTH + 1e-06)
    scaled = (features * in_gain).astype(jnp.bfloat16)
    projected = jnp.dot(scaled, in_weight, preferred_element_type=jnp.float32) * row_scale[:, None]
    projected = projected.reshape(SEQS, HEADS, PROJ)
    query_vec = projected[:, :, :KEY_DIM]
    key_vec = projected[:, :, KEY_DIM:2 * KEY_DIM]
    value_vec = projected[:, :, 2 * KEY_DIM:2 * KEY_DIM + VAL_DIM]
    gate_vec = projected[:, :, 2 * KEY_DIM + VAL_DIM:2 * KEY_DIM + 2 * VAL_DIM]
    logits = projected[:, :, 2 * KEY_DIM + 2 * VAL_DIM:] + level_bias[None]
    level_ids = jnp.arange(LEVELS, dtype=jnp.int32)
    occupied = occupancy(positions, level_ids) == 1
    peak_logit = lax.optimization_barrier(jnp.max(jnp.where(occupied, logits, -1e+30), axis=2, keepdims=True))
    weights = jnp.where(occupied, jnp.exp(logits - peak_logit), 0.0)
    total_weight = lax.optimization_barrier(jnp.sum(weights, axis=2))
    query_low = query_vec.astype(jnp.bfloat16)

    def read_head(head_id):
        query_head = lax.dynamic_index_in_dim(query_low, head_id, 1, keepdims=False).astype(jnp.float32)
        state_head = lax.dynamic_index_in_dim(states, head_id, 1, keepdims=False).astype(jnp.float32)
        return jnp.einsum('bk,blkv->blv', query_head, state_head)
    reads = lax.map(read_head, jnp.arange(HEADS, dtype=jnp.int32))
    reads = jnp.transpose(reads, (1, 0, 2, 3))
    own_term = lax.optimization_barrier(jnp.sum(query_vec * key_vec, axis=2, keepdims=True)) * KEY_DIM ** (-0.5) * value_vec
    mixed = lax.optimization_barrier(jnp.sum(weights[..., None] * reads, axis=2)) + weights[:, :, :1] * own_term
    level_out = mixed / total_weight[..., None]
    gated = (level_out * jax.nn.silu(gate_vec)).reshape(SEQS, HEADS * VAL_DIM)
    mean_square = lax.optimization_barrier(jnp.mean(gated * gated, axis=1, keepdims=True))
    normed = (gated * lax.rsqrt(mean_square + 1e-05) * out_gain).astype(jnp.bfloat16)
    return jnp.dot(normed, out_weight, preferred_element_type=jnp.float32)
```

```python
import functools

import jax
import jax.numpy as jnp
from jax import lax
from jax.experimental import pallas as pl
from jax.experimental.pallas import tpu as pltpu
from jax.sharding import PartitionSpec as P

LANES = 128
GROUP = 16


def send(src, dst, send_sem, recv_sem, target):
    return pltpu.make_async_remote_copy(
        src_ref=src,
        dst_ref=dst,
        send_sem=send_sem,
        recv_sem=recv_sem,
        device_id=target,
        device_id_type=pl.DeviceIdType.MESH,
    )


def arrived(shape_of, sem):
    pltpu.make_async_copy(shape_of, shape_of, sem).wait()


def kernel(
    heads, levels, width, dims,
    feat, gain_any, inw, bias_any, states, pos_any, ogain_any, outw, out,
    gain, bias, pos, ogain, xbuf, wbuf, sbuf, owbuf, proj, abuf, bbuf, mbuf, osend, orecv, qfull, wnorm, qw, biasbuf, qsum,
    small_sem, x_sem, w_sem, s_sem, ow_sem, p1_send, p1_recv, a_send, a_recv, b_send, b_recv,
    m_send, m_recv, o_send, o_recv, q_send, q_recv,
):
    key_dim, val_dim, level_total, level_here = dims
    seqs, fw = feat.shape
    flipped = fw % LANES == 0
    cols = inw.shape[0] if flipped else inw.shape[1]
    owned = seqs // levels
    out_rows = seqs // heads
    out_cols = outw.shape[1]
    me_h, me_l = lax.axis_index("head"), lax.axis_index("level")
    slot = 1 << level_total.bit_length()
    slots = LANES // slot
    packed = seqs // slots
    groups = seqs // GROUP

    x_copy = pltpu.make_async_copy(feat, xbuf.at[me_h], x_sem)
    x_copy.start()
    last_group = (me_l * owned) // GROUP
    order = [lax.rem(last_group + 1 + t, groups) for t in range(groups)]

    def state_copy(g):
        rows = pl.ds(pl.multiple_of(g * GROUP, GROUP), GROUP)
        return pltpu.make_async_copy(states.at[rows], sbuf.at[rows], s_sem.at[g])

    ow_copy = pltpu.make_async_copy(outw, owbuf, ow_sem)

    barrier = pltpu.get_barrier_semaphore()
    for o in range(1, heads):
        pl.semaphore_signal(
            barrier, inc=1, device_id=(lax.rem(me_h + o, heads), me_l),
            device_id_type=pl.DeviceIdType.MESH)
    for o in range(1, levels):
        pl.semaphore_signal(
            barrier, inc=1, device_id=(me_h, lax.rem(me_l + o, levels)),
            device_id_type=pl.DeviceIdType.MESH)
    smalls = [
        pltpu.make_async_copy(a, b, small_sem.at[i])
        for i, (a, b) in enumerate(((gain_any, gain), (bias_any, bias), (pos_any, pos), (ogain_any, ogain)))]
    for c in smalls:
        c.start()
    for h in range(heads):
        start = pl.multiple_of((h * levels + me_l) * fw, fw)
        part = inw.at[:, pl.ds(start, fw)] if flipped else inw.at[pl.ds(start, fw), :]
        pltpu.make_async_copy(part, wbuf.at[h], w_sem).start()
    pl.semaphore_wait(barrier, heads + levels - 2)

    x_copy.wait()
    buddy = me_h + 1 - 2 * lax.rem(me_h, 2)
    def feature_send(block, target, index):
        c = send(xbuf.at[block], xbuf.at[block], p1_send, p1_recv.at[block], (target, me_l))
        c.start()

    def feature_wait(block):
        send(xbuf.at[block], xbuf.at[block], p1_send, p1_recv.at[block], (buddy, me_l)).wait_recv()

    chips, core = heads // 2, lax.rem(me_h, 2)
    mirror_chip = chips - 1 - me_h // 2
    skip = lax.rem(me_h // 2 - mirror_chip + chips, chips)
    mirror = 2 * mirror_chip + core
    direct = []
    for j in range(1, chips - 1):
        near = 2 * lax.rem(mirror_chip + j + (j + chips - skip) // chips, chips)
        direct += [near + core, near + 1 - core]
    feature_send(me_h, mirror, heads - 1)
    for i, peer in enumerate(direct):
        feature_send(me_h, peer, i)
    feature_send(me_h, buddy, heads - 2)
    for c in smalls:
        c.wait()
    arrived(wbuf, w_sem)
    acc = jnp.zeros((seqs, cols), jnp.float32)
    squares = jnp.zeros((seqs, 1), jnp.float32)
    arrivals = [me_h, buddy, mirror] + direct + [2 * mirror_chip + 1 - core]
    for i, src in enumerate(arrivals):
        if i:
            feature_wait(src)
        if i == 2:
            feature_send(mirror, buddy, heads - 3)
        x = xbuf[src]
        g = gain[pl.ds(src * levels + me_l, 1), :]
        acc += lax.dot_general(
            (x * g).astype(jnp.bfloat16), wbuf[src], (((1,), (1 if flipped else 0,)), ((), ())),
            preferred_element_type=jnp.float32)
        squares += jnp.sum(x * x, axis=1, keepdims=True)

    for g in order:
        state_copy(g).start()
    ow_copy.start()

    proj[:, :cols] = acc
    lane = lax.broadcasted_iota(jnp.int32, (seqs, LANES), 1)
    tail0 = 2 * key_dim + 2 * val_dim
    tail = jnp.where(lane < level_total, proj[:, tail0 : tail0 + LANES], 0.0)
    tail = jnp.where(lane == level_total, squares, tail)
    pack = tail[:packed]
    for c in range(1, slots):
        pack += pltpu.roll(tail[c * packed : (c + 1) * packed], slot * c, 1)
    abuf[me_l, :seqs, :] = acc[:, :key_dim]
    abuf[me_l, seqs:, :] = pack
    for o in range(1, levels):
        peer = lax.rem(me_l + o, levels)
        c = send(abuf.at[me_l], abuf.at[me_l], a_send, a_recv, (me_h, peer))
        c.start()
    for o in range(1, levels):
        peer = lax.rem(me_l + o, levels)
        rows = pl.ds(pl.multiple_of(peer * owned, owned), owned)
        c = send(proj.at[rows, pl.ds(key_dim, tail0 - key_dim)], bbuf.at[me_l],
                 b_send, b_recv, (me_h, peer))
        c.start()
    mine = pl.ds(pl.multiple_of(me_l * owned, owned), owned)
    bbuf[me_l] = proj[mine, key_dim:tail0]

    biasbuf[:, :level_total] = bias[...]
    row = lax.broadcasted_iota(jnp.int32, (seqs, seqs), 0)
    col = lax.broadcasted_iota(jnp.int32, (seqs, seqs), 1)
    pos_f = jnp.broadcast_to(pos[...], (seqs, seqs)).astype(jnp.float32)
    pos_col = jnp.sum(jnp.where(row == col, pos_f, 0.0), axis=1, keepdims=True).astype(jnp.int32)
    shift = jnp.clip(lane - 1, 0, 31)
    bits = jnp.bitwise_and(jnp.right_shift(jnp.broadcast_to(pos_col, lane.shape), shift), 1)
    occupied = jnp.logical_and(lane < level_total, jnp.logical_or(lane == 0, bits == 1))

    arrived(abuf.at[pl.ds(0, levels - 1)], a_recv)
    query = abuf[0, :seqs, :]
    pack = abuf[0, seqs:, :]
    for l in range(1, levels):
        query += abuf[l, :seqs, :]
        pack += abuf[l, seqs:, :]
    parts = [pack] + [pltpu.roll(pack, LANES - slot * c, 1) for c in range(1, slots)]
    tail = jnp.concatenate(parts, axis=0)
    row_scale = lax.rsqrt(tail[:, level_total : level_total + 1] / width + 1e-06)
    query = query * row_scale
    logits = tail * row_scale + biasbuf[...]
    peak = jnp.max(jnp.where(occupied, logits, -1e30), axis=1, keepdims=True)
    weights = jnp.where(occupied, jnp.exp(logits - peak), 0.0)
    weights = weights / jnp.sum(weights, axis=1, keepdims=True)
    qfull[...] = query
    wnorm[:, :LANES] = weights
    wnorm[:, LANES:] = jnp.broadcast_to(row_scale, weights.shape)
    local = pltpu.roll(weights, lax.rem(LANES - me_l * level_here, LANES), 1)
    query_low = query.astype(jnp.bfloat16).astype(jnp.float32)
    for j in range(level_here):
        qw[:, j * key_dim : (j + 1) * key_dim] = (query_low * local[:, j : j + 1]).astype(jnp.bfloat16)

    seq_in = lax.broadcasted_iota(jnp.int32, (GROUP, val_dim), 0)
    def to_levels(rows):
        for o in range(1, levels):
            part = mbuf.at[me_l, rows, :]
            c = send(part, part, m_send, m_recv,
                     (me_h, lax.rem(me_l + o, levels)))
            c.start()

    for t, g in enumerate(order):
        if t == groups - 1:
            arrived(bbuf.at[pl.ds(0, levels - 1)], b_recv)
            rest = bbuf[0]
            for l in range(1, levels):
                rest += bbuf[l]
            rest = rest * wnorm[mine, LANES : LANES + 1]
            key, value = rest[:, :key_dim], rest[:, key_dim : key_dim + val_dim]
            gate = rest[:, key_dim + val_dim :]
            own = jnp.sum(qfull[mine, :] * key, axis=1, keepdims=True) * key_dim ** (-0.5) * value
            mbuf[me_l, seqs:, :] = gate * jax.nn.sigmoid(gate)
            to_levels(pl.ds(seqs, owned))
            qfull[...] = jnp.zeros(qfull.shape, jnp.float32)
            qfull[mine, :] = wnorm[mine, 0:1] * own
        state_copy(g).wait()
        base = pl.multiple_of(g * GROUP, GROUP)
        rows = pl.ds(base, GROUP)
        left = qw[rows, :]
        mixed = jnp.zeros((GROUP, val_dim), jnp.float32)
        for i in range(GROUP):
            got = jnp.dot(left, sbuf[base + i], preferred_element_type=jnp.float32)
            mixed = jnp.where(seq_in == i, got, mixed)
        if t == groups - 1:
            mixed += qfull[rows, :]
        mbuf[me_l, rows, :] = mixed
        to_levels(rows)
    ow_copy.wait()
    arrived(mbuf.at[pl.ds(0, levels - 1)], m_recv)
    gated = mbuf[0, :seqs, :]
    for l in range(1, levels):
        gated += mbuf[l, :seqs, :]
    gated = gated * jnp.concatenate([mbuf[l, seqs:, :] for l in range(levels)], axis=0)
    total_sq = jnp.sum(gated * gated, axis=1, keepdims=True)
    product = jnp.dot((gated * ogain[...]).astype(jnp.bfloat16), owbuf[...], preferred_element_type=jnp.float32)
    qsum[me_h] = jnp.sum(jnp.where(row == col, jnp.broadcast_to(total_sq, (seqs, seqs)), 0.0), axis=0, keepdims=True)
    for h in range(heads):
        osend[h] = product[h * out_rows : (h + 1) * out_rows]
    for o in range(1, heads):
        peer = lax.rem(me_h + o, heads)
        c = send(osend.at[peer], orecv.at[me_h], o_send, o_recv, (peer, me_l))
        c.start()
        c = send(qsum.at[me_h], qsum.at[me_h], q_send, q_recv, (peer, me_l))
        c.start()
    total = osend[me_h]
    arrived(orecv.at[pl.ds(0, heads - 1)], o_recv)
    arrived(qsum.at[pl.ds(0, heads - 1)], q_recv)
    for o in range(1, heads):
        total += orecv[lax.rem(me_h + heads - o, heads)]
    all_sq = qsum[0]
    for h in range(1, heads):
        all_sq += qsum[h]
    here = lax.broadcasted_iota(jnp.int32, (out_rows, seqs), 0) + me_h * out_rows
    pick = lax.broadcasted_iota(jnp.int32, (out_rows, seqs), 1) == here
    mean = jnp.sum(jnp.where(pick, jnp.broadcast_to(all_sq, pick.shape), 0.0), axis=1, keepdims=True) / (heads * val_dim)
    out[...] = total * lax.rsqrt(mean + 1e-05)
    arrived(xbuf.at[pl.ds(0, heads - 1)], p1_send)
    arrived(abuf.at[pl.ds(0, levels - 1)], a_send)
    arrived(bbuf.at[pl.ds(0, levels - 1)], b_send)
    arrived(mbuf.at[pl.ds(0, levels - 1)], m_send)
    arrived(orecv.at[pl.ds(0, heads - 1)], o_send)
    arrived(qsum.at[pl.ds(0, heads - 1)], q_send)


def body(features, in_gain, in_weight, level_bias, states, positions, out_gain, out_weight):
    heads, levels = lax.axis_size("head"), lax.axis_size("level")
    seqs, fw = features.shape
    cols = in_weight.shape[1]
    _, head_here, level_here, key_dim, val_dim = states.shape
    level_total = level_bias.shape[1]
    assert head_here == 1 and key_dim == LANES and val_dim == LANES
    out_cols = out_weight.shape[1]
    flipped = fw % LANES == 0
    slots = LANES // (1 << level_total.bit_length())
    owned, out_rows = seqs // levels, seqs // heads
    f32, bf16 = jnp.float32, jnp.bfloat16
    vmem, anyspace = pl.BlockSpec(memory_space=pltpu.VMEM), pl.BlockSpec(memory_space=pl.ANY)
    dma = pltpu.SemaphoreType.DMA
    tail0 = 2 * key_dim + 2 * val_dim
    return pl.pallas_call(
        functools.partial(kernel, heads, levels, in_gain.shape[0], (key_dim, val_dim, level_total, level_here)),
        out_shape=pltpu.VMEM((out_rows, out_cols), f32),
        in_specs=[anyspace] * 8,
        out_specs=vmem,
        scratch_shapes=[
            pltpu.VMEM((heads * levels, fw), f32),
            pltpu.VMEM(level_bias.shape, f32),
            pltpu.VMEM((1, seqs), jnp.int32),
            pltpu.VMEM((1, val_dim), f32),
            pltpu.VMEM((heads, seqs, fw), f32),
            pltpu.VMEM((heads, cols, fw) if flipped else (heads, fw, cols), bf16),
            pltpu.VMEM((seqs, level_here * key_dim, val_dim), bf16),
            pltpu.VMEM(out_weight.shape, bf16),
            pltpu.VMEM((seqs, tail0 + LANES), f32),
            pltpu.VMEM((levels, seqs + seqs // slots, key_dim), f32),
            pltpu.VMEM((levels, owned, tail0 - key_dim), f32),
            pltpu.VMEM((levels, seqs + owned, val_dim), f32),
            pltpu.VMEM((heads, out_rows, out_cols), f32),
            pltpu.VMEM((heads, out_rows, out_cols), f32),
            pltpu.VMEM((seqs, key_dim), f32),
            pltpu.VMEM((seqs, 2 * LANES), f32),
            pltpu.VMEM((seqs, level_here * key_dim), bf16),
            pltpu.VMEM((1, LANES), f32),
            pltpu.VMEM((heads, 1, seqs), f32),
            dma((4,)), dma(()), dma(()), dma((seqs // GROUP,)), dma(()),
            dma(()), dma((heads,)),
            *[dma(())] * 10,
        ],
        compiler_params=pltpu.CompilerParams(collective_id=0, has_side_effects=True),
    )(
        features,
        in_gain.reshape(heads * levels, fw),
        in_weight.T if flipped else in_weight,
        level_bias,
        states.reshape(seqs, level_here * key_dim, val_dim),
        positions.reshape(1, seqs),
        out_gain.reshape(1, val_dim),
        out_weight,
    )


def solution(mesh):
    in_specs = (
        P(None, ("head", "level")),
        P(),
        P(None, "head"),
        P("head", None),
        P(None, "head", "level", None, None),
        P(),
        P("head"),
        P("head", "level"),
    )
    out_specs = P("head", "level")
    return jax.shard_map(body, mesh=mesh, in_specs=in_specs, out_specs=out_specs, check_vma=False)
```

```python
import functools

import jax
import jax.numpy as jnp
from jax import lax
from jax.experimental import pallas as pl
from jax.experimental.pallas import tpu as pltpu
from jax.sharding import PartitionSpec as P

LANES = 128
GROUP = 16


def send(src, dst, send_sem, recv_sem, target):
    c = pltpu.make_async_remote_copy(
        src_ref=src,
        dst_ref=dst,
        send_sem=send_sem,
        recv_sem=recv_sem,
        device_id=target,
        device_id_type=pl.DeviceIdType.MESH,
    )
    c.start()


def arrived(like, sem):
    pltpu.make_async_copy(like, like, sem).wait()


def flip_bits(value, mask, count):
    result, bit = 0, 1
    while bit < count:
        own = lax.rem(value // bit, 2)
        result = result + bit * (1 - own if mask & bit else own)
        bit *= 2
    return result


def kernel(
    heads, levels, width, dims,
    feat, gain_any, inw, bias_any, states, pos_any, ogain_any, outw, out,
    gain, bias, pos, ogain, xbuf, wbuf, sbuf, owbuf, tailbuf, tbuf, qbuf, kx, xk, keys, values, gates,
    wexp, scales, mbuf, osend, orecv, biasbuf,
    small_sem, x_sem, w_sem, s_sem, ow_sem, f_send, f_recv, kx_send, kx_recv, k2_send, k2_recv,
    t_send, t_recv, q_send, q_recv, g_send, g_recv, m_send, m_recv, o_send, o_recv,
):
    key_dim, val_dim, level_total, level_here = dims
    seqs, fw = feat.shape
    flipped = fw % LANES == 0
    owned = seqs // levels
    out_rows = seqs // heads
    out_cols = outw.shape[1]
    me_h, me_l = lax.axis_index("head"), lax.axis_index("level")
    slot = 1 << level_total.bit_length()
    slots = LANES // slot
    packed = seqs // slots
    groups = seqs // GROUP
    per = heads // groups
    block, me_j = me_h // per, lax.rem(me_h, per)
    order = [flip_bits(block, groups - 1 - t, groups) for t in range(groups)]
    mine = pl.ds(pl.multiple_of(me_l * owned, owned), owned)
    peers = [lax.rem(me_l + o, levels) for o in range(1, levels)]
    tail0 = 2 * key_dim + 2 * val_dim
    f32, bf16 = jnp.float32, jnp.bfloat16

    def group_rows(t):
        return pl.ds(pl.multiple_of(order[t] * GROUP, GROUP), GROUP)

    x_copy = pltpu.make_async_copy(feat, xbuf.at[me_h], x_sem)
    x_copy.start()

    barrier = pltpu.get_barrier_semaphore()
    for o in range(1, heads):
        pl.semaphore_signal(
            barrier, inc=1, device_id=(lax.rem(me_h + o, heads), me_l),
            device_id_type=pl.DeviceIdType.MESH)
    for peer in peers:
        pl.semaphore_signal(
            barrier, inc=1, device_id=(me_h, peer), device_id_type=pl.DeviceIdType.MESH)
    smalls = [
        pltpu.make_async_copy(a, b, small_sem.at[i])
        for i, (a, b) in enumerate(((gain_any, gain), (bias_any, bias), (pos_any, pos), (ogain_any, ogain)))]
    for c in smalls:
        c.start()
    w_copy = pltpu.make_async_copy(inw, wbuf, w_sem)
    w_copy.start()
    pl.semaphore_wait(barrier, heads + levels - 2)

    x_copy.wait()
    buddy = me_h + 1 - 2 * lax.rem(me_h, 2)

    def feature_send(source, target):
        send(xbuf.at[source], xbuf.at[source], f_send, f_recv.at[source], (target, me_l))

    def feature_wait(source):
        arrived(xbuf.at[source], f_recv.at[source])

    chips, core = heads // 2, lax.rem(me_h, 2)
    mirror_chip = chips - 1 - me_h // 2
    skip = lax.rem(me_h // 2 - mirror_chip + chips, chips)
    mirror = 2 * mirror_chip + core
    direct = []
    for j in range(1, chips - 1):
        near = 2 * lax.rem(mirror_chip + j + (j + chips - skip) // chips, chips)
        direct += [near + core, near + 1 - core]
    feature_send(me_h, mirror)
    for peer in direct:
        feature_send(me_h, peer)
    feature_send(me_h, buddy)
    for o, peer in enumerate(peers, 1):
        theirs = pl.ds(pl.multiple_of(peer * owned, owned), owned)
        send(xbuf.at[me_h, theirs], kx.at[levels - 1 - o, me_h], kx_send, kx_recv, (me_h, peer))
    for c in smalls:
        c.wait()
    w_copy.wait()

    def weight(first, last, start, size):
        if flipped:
            return wbuf[first:last, pl.ds(start, size)]
        return wbuf[pl.ds(start, size), first:last]

    def project(x, w):
        return lax.dot_general(x, w, (((1,), (1 if flipped else 0,)), ((), ())), preferred_element_type=f32)

    query = jnp.zeros((seqs, key_dim), f32)
    tail = jnp.zeros((seqs, level_total), f32)
    squares = jnp.zeros((seqs, fw), f32)
    arrivals = [me_h, buddy, mirror] + direct + [2 * mirror_chip + 1 - core]
    for i, src in enumerate(arrivals):
        if i:
            feature_wait(src)
        if i == 2:
            feature_send(mirror, buddy)
        x = xbuf[src]
        index = src * levels + me_l
        start = pl.multiple_of(index * fw, fw)
        scaled = (x * gain[pl.ds(index, 1), :]).astype(bf16)
        query += project(scaled, weight(0, key_dim, start, fw))
        tail += project(scaled, weight(tail0, tail0 + level_total, start, fw))
        squares += x * x
    squares = jnp.sum(squares, axis=1, keepdims=True)

    tailbuf[:, :level_total] = tail
    lane = lax.broadcasted_iota(jnp.int32, (seqs, LANES), 1)
    tail = jnp.where(lane < level_total, tailbuf[...], 0.0)
    tail = jnp.where(lane == level_total, squares, tail)
    pack = tail[:packed]
    for c in range(1, slots):
        pack += pltpu.roll(tail[c * packed : (c + 1) * packed], slot * c, 1)
    tbuf[me_l] = pack
    qbuf[me_l] = query
    for peer in peers:
        send(tbuf.at[me_l], tbuf.at[me_l], t_send, t_recv, (me_h, peer))
    for t in range(groups):
        part = qbuf.at[me_l, group_rows(t)]
        for peer in peers:
            send(part, part, q_send, q_recv.at[t], (me_h, peer))

    arrived(kx.at[:, 0], kx_recv)
    for o in range(1, heads):
        part = kx.at[:, me_h]
        send(part, part, k2_send, k2_recv, (lax.rem(me_h + o, heads), me_l))

    def state_copy(t):
        rows = group_rows(t)
        return pltpu.make_async_copy(states.at[rows], sbuf.at[rows], s_sem.at[t])

    for t in range(groups):
        state_copy(t).start()
    ow_copy = pltpu.make_async_copy(outw, owbuf, ow_sem)
    ow_copy.start()

    keys[...] = jnp.zeros(keys.shape, f32)
    values[...] = jnp.zeros(values.shape, f32)
    biasbuf[:, :level_total] = bias[...]
    row = lax.broadcasted_iota(jnp.int32, (seqs, seqs), 0)
    col = lax.broadcasted_iota(jnp.int32, (seqs, seqs), 1)
    pos_f = jnp.broadcast_to(pos[...], (seqs, seqs)).astype(f32)
    pos_col = jnp.sum(jnp.where(row == col, pos_f, 0.0), axis=1, keepdims=True).astype(jnp.int32)
    shift = jnp.clip(lane - 1, 0, 31)
    bits = jnp.bitwise_and(jnp.right_shift(jnp.broadcast_to(pos_col, lane.shape), shift), 1)
    occupied = jnp.logical_and(lane < level_total, jnp.logical_or(lane == 0, bits == 1))

    arrived(tbuf.at[pl.ds(0, levels - 1)], t_recv)
    pack = tbuf[0]
    for l in range(1, levels):
        pack += tbuf[l]
    parts = [pack] + [pltpu.roll(pack, LANES - slot * c, 1) for c in range(1, slots)]
    tail = jnp.concatenate(parts, axis=0)
    row_scale = lax.rsqrt(tail[:, level_total : level_total + 1] / width + 1e-06)
    logits = tail * row_scale + biasbuf[...]
    peak = jnp.max(jnp.where(occupied, logits, -1e30), axis=1, keepdims=True)
    weights = jnp.where(occupied, jnp.exp(logits - peak), 0.0)
    weights = weights / jnp.sum(weights, axis=1, keepdims=True)
    local = pltpu.roll(weights, lax.rem(LANES - me_l * level_here, LANES), 1)
    for j in range(level_here):
        wexp[:, j * key_dim : (j + 1) * key_dim] = jnp.broadcast_to(local[:, j : j + 1], (seqs, key_dim))
    scales[:, :LANES] = jnp.broadcast_to(row_scale, weights.shape)
    scales[:, LANES:] = jnp.broadcast_to(weights[:, :1], weights.shape)

    arrived(kx.at[:, pl.ds(0, heads - 1)], k2_recv)
    if flipped:
        squares = jnp.zeros((owned, fw), f32)
        for h in range(heads):
            for o in range(levels):
                x = kx[o - 1, h] if o else xbuf[h, mine, :]
                index = h * levels + lax.rem(me_l + o, levels)
                xk[:, pl.ds(pl.multiple_of(index * fw, fw), fw)] = (x * gain[pl.ds(index, 1), :]).astype(bf16)
                squares += x * x
        rest = project(xk[...], wbuf[key_dim:tail0, :])
    else:
        def part(h, carry):
            rest, squares = carry
            for o in range(levels):
                x = kx[o - 1, h] if o else xbuf[h, mine, :]
                index = h * levels + lax.rem(me_l + o, levels)
                start = pl.multiple_of(index * fw, fw)
                scaled = (x * gain[pl.ds(index, 1), :]).astype(bf16)
                rest = rest + project(scaled, weight(key_dim, tail0, start, fw))
                squares = squares + x * x
            return rest, squares

        rest, squares = lax.fori_loop(
            0, heads, part, (jnp.zeros((owned, tail0 - key_dim), f32), jnp.zeros((owned, fw), f32)))
    rest = rest * lax.rsqrt(jnp.sum(squares, axis=1, keepdims=True) / width + 1e-06)
    gate = rest[:, key_dim + val_dim :]
    keys[mine, :] = rest[:, :key_dim]
    values[mine, :] = rest[:, key_dim : key_dim + val_dim] * key_dim ** (-0.5)
    gates[mine, :] = gate * jax.nn.sigmoid(gate)
    for peer in peers:
        send(gates.at[mine], gates.at[mine], g_send, g_recv, (me_h, peer))

    seq_in = lax.broadcasted_iota(jnp.int32, (GROUP, val_dim), 0)
    for t in range(groups):
        rows = group_rows(t)
        arrived(qbuf.at[pl.ds(0, levels - 1), pl.ds(0, GROUP)], q_recv.at[t])
        query = qbuf[0, rows, :]
        for l in range(1, levels):
            query += qbuf[l, rows, :]
        query = query * scales[rows, :LANES]
        low = query.astype(bf16).astype(f32)
        left = jnp.concatenate(
            [(low * wexp[rows, j * key_dim : (j + 1) * key_dim]).astype(bf16) for j in range(level_here)], axis=1)
        own = jnp.sum(query * keys[rows, :], axis=1, keepdims=True) * values[rows, :]
        mixed = scales[rows, LANES:] * own
        state_copy(t).wait()
        base = pl.multiple_of(order[t] * GROUP, GROUP)
        reads = jnp.zeros((GROUP, val_dim), f32)
        for i in range(GROUP):
            got = jnp.dot(left, sbuf[base + i], preferred_element_type=f32)
            reads = jnp.where(seq_in == i, got, reads)
        mbuf[me_l, rows, :] = mixed + reads
        part = mbuf.at[me_l, rows]
        for peer in peers:
            send(part, part, m_send, m_recv.at[t], (me_h, peer))

    ow_copy.wait()
    arrived(gates.at[pl.ds(0, seqs - owned)], g_recv)
    for t in range(groups):
        rows = group_rows(t)
        arrived(mbuf.at[pl.ds(0, levels - 1), pl.ds(0, GROUP)], m_recv.at[t])
        gated = mbuf[0, rows, :]
        for l in range(1, levels):
            gated += mbuf[l, rows, :]
        gated = gated * gates[rows, :]
        total_sq = jnp.broadcast_to(jnp.sum(gated * gated, axis=1, keepdims=True), (GROUP, LANES))
        product = jnp.dot((gated * ogain[...]).astype(bf16), owbuf[...], preferred_element_type=f32)
        for j in range(per):
            osend[t, j, :, :out_cols] = product[j * out_rows : (j + 1) * out_rows]
            osend[t, j, :, out_cols:] = total_sq[j * out_rows : (j + 1) * out_rows]
        if t < groups - 1:
            for j in range(per):
                send(osend.at[t, j], orecv.at[me_h], o_send, o_recv, (order[t] * per + j, me_l))
        else:
            for o in range(1, per):
                j = lax.rem(me_j + o, per)
                send(osend.at[t, j], orecv.at[me_h], o_send, o_recv, (block * per + j, me_l))
    total = osend[groups - 1, me_j]
    arrived(orecv.at[pl.ds(0, heads - 1)], o_recv)
    for o in range(1, heads):
        total += orecv[lax.rem(me_h + heads - o, heads)]
    mean = total[:, out_cols : out_cols + 1] / (heads * val_dim)
    out[...] = total[:, :out_cols] * lax.rsqrt(mean + 1e-05)
    arrived(xbuf.at[pl.ds(0, heads - 1)], f_send)
    arrived(kx.at[:, 0], kx_send)
    arrived(kx.at[:, pl.ds(0, heads - 1)], k2_send)
    arrived(tbuf.at[pl.ds(0, levels - 1)], t_send)
    arrived(qbuf.at[pl.ds(0, levels - 1)], q_send)
    arrived(gates.at[pl.ds(0, seqs - owned)], g_send)
    arrived(mbuf.at[pl.ds(0, levels - 1)], m_send)
    arrived(orecv.at[pl.ds(0, heads - 1)], o_send)


def body(features, in_gain, in_weight, level_bias, states, positions, out_gain, out_weight):
    heads, levels = lax.axis_size("head"), lax.axis_size("level")
    seqs, fw = features.shape
    width, cols = in_weight.shape
    _, head_here, level_here, key_dim, val_dim = states.shape
    level_total = level_bias.shape[1]
    assert head_here == 1 and key_dim == LANES and val_dim == LANES
    out_cols = out_weight.shape[1]
    flipped = fw % LANES == 0
    slots = LANES // (1 << level_total.bit_length())
    owned, out_rows, groups = seqs // levels, seqs // heads, seqs // GROUP
    f32, bf16 = jnp.float32, jnp.bfloat16
    vmem, anyspace = pl.BlockSpec(memory_space=pltpu.VMEM), pl.BlockSpec(memory_space=pl.ANY)
    dma = pltpu.SemaphoreType.DMA
    return pl.pallas_call(
        functools.partial(kernel, heads, levels, in_gain.shape[0], (key_dim, val_dim, level_total, level_here)),
        out_shape=pltpu.VMEM((out_rows, out_cols), f32),
        in_specs=[anyspace] * 8,
        out_specs=vmem,
        scratch_shapes=[
            pltpu.VMEM((heads * levels, fw), f32),
            pltpu.VMEM(level_bias.shape, f32),
            pltpu.VMEM((1, seqs), jnp.int32),
            pltpu.VMEM((1, val_dim), f32),
            pltpu.VMEM((heads, seqs, fw), f32),
            pltpu.VMEM((cols, width) if flipped else (width, cols), bf16),
            pltpu.VMEM((seqs, level_here * key_dim, val_dim), bf16),
            pltpu.VMEM(out_weight.shape, bf16),
            pltpu.VMEM((seqs, LANES), f32),
            pltpu.VMEM((levels, seqs // slots, LANES), f32),
            pltpu.VMEM((levels, seqs, key_dim), f32),
            pltpu.VMEM((levels - 1, heads, owned, fw), f32),
            pltpu.VMEM((owned, width), bf16),
            pltpu.VMEM((seqs, key_dim), f32),
            pltpu.VMEM((seqs, val_dim), f32),
            pltpu.VMEM((seqs, val_dim), f32),
            pltpu.VMEM((seqs, level_here * key_dim), f32),
            pltpu.VMEM((seqs, 2 * LANES), f32),
            pltpu.VMEM((levels, seqs, val_dim), f32),
            pltpu.VMEM((groups, heads // groups, out_rows, out_cols + LANES), f32),
            pltpu.VMEM((heads, out_rows, out_cols + LANES), f32),
            pltpu.VMEM((1, LANES), f32),
            dma((4,)), dma(()), dma(()), dma((groups,)), dma(()),
            dma(()), dma((heads,)), *[dma(())] * 4,
            dma(()), dma(()), dma(()), dma((groups,)), dma(()), dma(()), dma(()), dma((groups,)), dma(()), dma(()),
        ],
        compiler_params=pltpu.CompilerParams(collective_id=0, has_side_effects=True),
    )(
        features,
        in_gain.reshape(heads * levels, fw),
        in_weight.T if flipped else in_weight,
        level_bias,
        states.reshape(seqs, level_here * key_dim, val_dim),
        positions.reshape(1, seqs),
        out_gain.reshape(1, val_dim),
        out_weight,
    )


def solution(mesh):
    in_specs = (
        P(None, ("head", "level")),
        P(),
        P(None, "head"),
        P("head", None),
        P(None, "head", "level", None, None),
        P(),
        P("head"),
        P("head", "level"),
    )
    out_specs = P("head", "level")
    return jax.shard_map(body, mesh=mesh, in_specs=in_specs, out_specs=out_specs, check_vma=False)
```

```python
import functools

import jax
import jax.numpy as jnp
from jax import lax
from jax.experimental import pallas as pl
from jax.experimental.pallas import tpu as pltpu
from jax.sharding import PartitionSpec as P

LANES = 128
GROUP = 16
POSITION_BITS = 18


def send(src, dst, send_sem, recv_sem, target):
    c = pltpu.make_async_remote_copy(
        src_ref=src,
        dst_ref=dst,
        send_sem=send_sem,
        recv_sem=recv_sem,
        device_id=target,
        device_id_type=pl.DeviceIdType.MESH,
    )
    c.start()


def arrived(like, sem):
    pltpu.make_async_copy(like, like, sem).wait()


def exclusive_or(a, b, count):
    result, bit = 0, 1
    while bit < count:
        result = result + bit * lax.rem(a // bit + b // bit, 2)
        bit *= 2
    return result


def kernel(
    heads, levels, width, dims,
    feat, gain_any, inw, bias_any, states, pos_any, ogain_any, outw, out,
    gain, bias, pos, ogain, xbuf, wbuf, sbuf, owbuf, tailbuf, tbuf, qbuf, qtmp, kx, gates, restbuf, sqbuf, ownbuf,
    wexp, scales, mbuf, osend, orecv, biasbuf,
    z_sem, small_sem, x_sem, w_sem, s_sem, ow_sem, sent, f_recv, kx_recv, k2_recv,
    t_recv, q_recv, g_recv, m_recv, o_recv,
):
    key_dim, val_dim, level_total, level_here = dims
    seqs, fw = feat.shape
    flipped = fw % LANES == 0
    owned = seqs // levels
    out_rows = seqs // heads
    out_cols = outw.shape[1]
    me_h, me_l = lax.axis_index("head"), lax.axis_index("level")
    slot = 1 << level_total.bit_length()
    slots = LANES // slot
    packed = seqs // slots
    groups = seqs // GROUP
    per = heads // groups
    block, me_j = me_h // per, lax.rem(me_h, per)
    order = [exclusive_or(block, groups - 1 - t, groups) for t in range(groups)]
    my_block = me_l * owned // GROUP
    my_t = groups - 1 - exclusive_or(block, my_block, groups)
    own_rows = pl.ds(pl.multiple_of(my_t * GROUP + lax.rem(me_l * owned, GROUP), owned), owned)
    mine = pl.ds(pl.multiple_of(me_l * owned, owned), owned)
    peers = [l + jnp.where(me_l <= l, 1, 0) for l in range(levels - 1)]

    def by_level(choice):
        value = jnp.int32(choice(0))
        for l in range(1, levels):
            value = jnp.where(me_l == l, choice(l), value)
        return value

    tail0 = 2 * key_dim + 2 * val_dim
    f32, bf16 = jnp.float32, jnp.bfloat16

    def group_rows(t):
        return pl.ds(pl.multiple_of(order[t] * GROUP, GROUP), GROUP)

    def rows_of_group(ref, t, first=0, last=LANES):
        return ref[group_rows(t), first:last]

    x_copy = pltpu.make_async_copy(feat, xbuf.at[me_h], x_sem)
    x_copy.start()

    def tell(sem, h, l):
        pl.semaphore_signal(sem, inc=1, device_id=(h, l), device_id_type=pl.DeviceIdType.MESH)

    core = lax.rem(me_h, 2)
    buddy = me_h + 1 - 2 * core
    barrier = pltpu.get_barrier_semaphore()
    pl.loop(me_l + 1, levels)(lambda l: tell(barrier, me_h, l))
    for o in range(1, heads):
        tell(barrier, lax.rem(me_h + o, heads), me_l)
    smalls = [
        pltpu.make_async_copy(a, b, small_sem.at[i])
        for i, (a, b) in enumerate(((gain_any, gain), (bias_any, bias), (pos_any, pos), (ogain_any, ogain)))]
    for c in smalls:
        c.start()
    if flipped:
        for l in range(levels):
            for h in range(heads):
                pltpu.make_async_copy(
                    inw.at[:, pl.ds((h * levels + l) * fw, fw)], wbuf.at[:, pl.ds((l * heads + h) * fw, fw)], w_sem).start()
    else:
        pltpu.make_async_copy(inw, wbuf, w_sem).start()
    pl.semaphore_wait(barrier, heads - 1 + me_l)
    pl.loop(0, me_l)(lambda l: tell(z_sem, me_h, l))

    x_copy.wait()

    def feature_send(source, target):
        send(xbuf.at[source], xbuf.at[source], sent, f_recv.at[source], (target, me_l))

    def feature_wait(source):
        arrived(xbuf.at[source], f_recv.at[source])

    chips = heads // 2
    mirror_chip = chips - 1 - me_h // 2
    skip = lax.rem(me_h // 2 - mirror_chip + chips, chips)
    mirror = 2 * mirror_chip + core
    direct = []
    for j in range(1, chips - 1):
        near = 2 * lax.rem(mirror_chip + j + (j + chips - skip) // chips, chips)
        direct += [near + core, near + 1 - core]
    feature_send(me_h, mirror)
    for peer in direct:
        feature_send(me_h, peer)
    feature_send(me_h, buddy)

    def rows_send(l):
        theirs = pl.ds(pl.multiple_of(l * owned, owned), owned)
        send(xbuf.at[me_h, theirs], kx.at[me_l, me_h], sent, kx_recv.at[me_l], (me_h, l))

    pl.loop(0, me_l)(rows_send)
    for c in smalls:
        c.wait()
    arrived(wbuf, w_sem)

    def weight(first, last, h, l):
        if flipped:
            return wbuf[first:last, pl.ds(pl.multiple_of((l * heads + h) * fw, fw), fw)]
        return wbuf[pl.ds(pl.multiple_of((h * levels + l) * fw, fw), fw), first:last]

    def project(x, w):
        return lax.dot_general(x, w, (((1,), (1 if flipped else 0,)), ((), ())), preferred_element_type=f32)

    query = jnp.zeros((seqs, key_dim), f32)
    tail = jnp.zeros((seqs, level_total), f32)
    squares = jnp.zeros((seqs, fw), f32)
    arrivals = [me_h, buddy, mirror] + direct + [2 * mirror_chip + 1 - core]
    for i, src in enumerate(arrivals):
        if i == len(arrivals) - 2:
            @pl.when(me_l < levels - 1)
            def _():
                pl.semaphore_wait(z_sem, levels - 1 - me_l)

            pl.loop(me_l + 1, levels)(rows_send)
        if i:
            feature_wait(src)
        if i == 2:
            feature_send(mirror, buddy)
        x = xbuf[src]
        index = src * levels + me_l
        scaled = (x * gain[pl.ds(index, 1), :]).astype(bf16)
        query += project(scaled, weight(0, key_dim, src, me_l))
        tail += project(scaled, weight(tail0, tail0 + level_total, src, me_l))
        squares += x * x
    squares = jnp.sum(squares, axis=1, keepdims=True)

    tailbuf[:, :level_total] = tail
    lane = lax.broadcasted_iota(jnp.int32, (seqs, LANES), 1)
    tail = jnp.where(lane < level_total, tailbuf[...], 0.0)
    tail = jnp.where(lane == level_total, squares, tail)
    pack = tail[:packed]
    for c in range(1, slots):
        pack += pltpu.roll(tail[c * packed : (c + 1) * packed], slot * c, 1)
    tbuf[me_l] = pack
    qtmp[...] = query
    for t in range(groups):
        qbuf[me_l, t * GROUP : (t + 1) * GROUP] = rows_of_group(qtmp, t)
    for peer in peers:
        send(tbuf.at[me_l], tbuf.at[me_l], sent, t_recv, (me_h, peer))
    for t in range(groups):
        part = qbuf.at[me_l, pl.ds(t * GROUP, GROUP)]
        for peer in peers:
            send(part, part, sent, q_recv.at[t], (me_h, peer))

    possible = min(level_total, POSITION_BITS + 1)
    counts = sorted({min(max(possible - l * level_here, 0), level_here) for l in range(levels)})
    count = jnp.clip(possible - me_l * level_here, 0, level_here)

    def state_start(t, n):
        part = (group_rows(t), pl.ds(0, n * key_dim))
        pltpu.make_async_copy(states.at[part], sbuf.at[part], s_sem).start()

    for n in counts:
        @pl.when(jnp.logical_and(count == n, n > 0))
        def _():
            for t in range(groups):
                state_start(t, n)

    ow_copy = pltpu.make_async_copy(outw, owbuf, ow_sem)
    ow_copy.start()

    biasbuf[:, :level_total] = bias[...]
    row = lax.broadcasted_iota(jnp.int32, (seqs, seqs), 0)
    col = lax.broadcasted_iota(jnp.int32, (seqs, seqs), 1)
    pos_f = jnp.broadcast_to(pos[...], (seqs, seqs)).astype(f32)
    pos_col = jnp.sum(jnp.where(row == col, pos_f, 0.0), axis=1, keepdims=True).astype(jnp.int32)
    shift = jnp.clip(lane - 1, 0, 31)
    bits = jnp.bitwise_and(jnp.right_shift(jnp.broadcast_to(pos_col, lane.shape), shift), 1)
    occupied = jnp.logical_and(lane < level_total, jnp.logical_or(lane == 0, bits == 1))

    def piece(l, rows_of):
        total = jnp.zeros((owned, fw), f32)
        if flipped:
            scaled = []
            for h in range(heads):
                x = rows_of(h)
                scaled.append((x * gain[pl.ds(h * levels + l, 1), :]).astype(bf16))
                total += x * x
            at = pl.ds(pl.multiple_of(l * heads * fw, heads * fw), heads * fw)
            return project(jnp.concatenate(scaled, axis=1), wbuf[key_dim:tail0, at]), total

        def step(h, carry):
            rest, total = carry
            x = rows_of(h)
            scaled = (x * gain[pl.ds(h * levels + l, 1), :]).astype(bf16)
            return rest + project(scaled, weight(key_dim, tail0, h, l)), total + x * x

        return lax.fori_loop(0, heads, step, (jnp.zeros((owned, tail0 - key_dim), f32), total))

    restbuf[...], sqbuf[...] = piece(me_l, lambda h: xbuf[h, mine, :])
    for s in range(levels - 1):
        l = by_level(lambda me: sorted((p for p in range(levels) if p != me), key=lambda p: (abs(p - me), p))[s])
        arrived(kx.at[0, 0], kx_recv.at[l])
        part = kx.at[l, me_h]
        for target in [mirror, 2 * mirror_chip + 1 - core] + direct + [buddy]:
            send(part, part, sent, k2_recv, (target, me_l))

    arrived(tbuf.at[pl.ds(0, levels - 1)], t_recv)
    pack = tbuf[0]
    for l in range(1, levels):
        pack += tbuf[l]
    parts = [pack] + [pltpu.roll(pack, LANES - slot * c, 1) for c in range(1, slots)]
    tail = jnp.concatenate(parts, axis=0)
    row_scale = lax.rsqrt(tail[:, level_total : level_total + 1] / width + 1e-06)
    logits = tail * row_scale + biasbuf[...]
    peak = jnp.max(jnp.where(occupied, logits, -1e30), axis=1, keepdims=True)
    weights = jnp.where(occupied, jnp.exp(logits - peak), 0.0)
    weights = weights / jnp.sum(weights, axis=1, keepdims=True)
    local = pltpu.roll(weights, lax.rem(LANES - me_l * level_here, LANES), 1)
    for j in range(level_here):
        wexp[:, j * key_dim : (j + 1) * key_dim] = jnp.broadcast_to(local[:, j : j + 1], (seqs, key_dim))
    scales[:, :LANES] = jnp.broadcast_to(row_scale, weights.shape)
    scales[:, LANES:] = jnp.broadcast_to(weights[:, :1], weights.shape)

    def query_wait(t):
        arrived(qbuf.at[pl.ds(0, levels - 1), pl.ds(0, GROUP)], q_recv.at[t])

    def own_and_gate(last):
        rest, squares = restbuf[...], sqbuf[...]
        arrived(kx.at[pl.ds(0, levels - 1), pl.ds(0, heads - 1)], k2_recv)
        for l in peers:
            more = piece(l, lambda h: kx[l, h])
            rest, squares = rest + more[0], squares + more[1]
        rest = rest * lax.rsqrt(jnp.sum(squares, axis=1, keepdims=True) / width + 1e-06)
        key, value, gate = [rest[:, j * key_dim : (j + 1) * key_dim] for j in range(3)]
        gates[mine, :] = gate * jax.nn.sigmoid(gate)
        for peer in peers:
            send(gates.at[mine], gates.at[mine], sent, g_recv.at[me_l], (me_h, peer))
        if last:
            query_wait(groups - 1)
        query = qbuf[0, own_rows, :]
        for l in range(1, levels):
            query += qbuf[l, own_rows, :]
        query = query * scales[mine, :LANES]
        own = jnp.sum(query * key, axis=1, keepdims=True) * key_dim ** (-0.5) * value
        ownbuf[...] = scales[mine, LANES:] * own

    def own_send():
        mbuf[me_l, own_rows, :] += ownbuf[...]
        reads_send(my_t)

    seq_in = lax.broadcasted_iota(jnp.int32, (GROUP, val_dim), 0)
    def reads_send(t):
        part = mbuf.at[me_l, pl.ds(pl.multiple_of(t * GROUP, GROUP), GROUP)]
        for peer in peers:
            send(part, part, sent, m_recv.at[t], (me_h, peer))

    def read_group(t, n):
        here = pl.ds(t * GROUP, GROUP)
        reads = jnp.zeros((GROUP, val_dim), f32)
        if n:
            query = qbuf[0, here, :]
            for l in range(1, levels):
                query += qbuf[l, here, :]
            low = (query * rows_of_group(scales, t)).astype(bf16).astype(f32)
            left = jnp.concatenate(
                [(low * rows_of_group(wexp, t, j * key_dim, (j + 1) * key_dim)).astype(bf16) for j in range(n)], axis=1)
            for i in range(GROUP):
                seq = order[t] * GROUP + i
                got = jnp.dot(left, sbuf[seq, : n * key_dim, :], preferred_element_type=f32)
                reads = jnp.where(seq_in == i, got, reads)
        mbuf[me_l, here, :] = reads

        @pl.when(order[t] != my_block)
        def _():
            reads_send(t)

    for n in counts:
        @pl.when(count == n)
        def _():
            if n:
                arrived(sbuf.at[:, pl.ds(0, n * key_dim)], s_sem)
            for t in range(groups - 1):
                query_wait(t)
                read_group(t, n)
            if n < level_here:
                query_wait(groups - 1)
                read_group(groups - 1, n)
            own_and_gate(n == level_here)
            if n < level_here:
                own_send()
            else:
                pl.when(my_t < groups - 1)(own_send)
                read_group(groups - 1, n)
                pl.when(my_t == groups - 1)(own_send)

    def nearest(l, own, s):
        return sorted(range(groups), key=lambda b: (b == own, abs((2 * b + 1) * levels - (2 * l + 1) * groups), b))[s]

    ow_copy.wait()
    for s in range(groups):
        b = by_level(lambda l: nearest(l, 0, s))
        for own in range(1, groups):
            b = jnp.where(block == own, by_level(lambda l: nearest(l, own, s)), b)
        t = groups - 1 - exclusive_or(block, b, groups)
        for o in range(GROUP // owned):
            owner = b * (GROUP // owned) + o

            @pl.when(owner != me_l)
            def _():
                arrived(gates.at[pl.ds(0, owned)], g_recv.at[owner])

        arrived(mbuf.at[pl.ds(0, levels - 1), pl.ds(0, GROUP)], m_recv.at[t])
        here = pl.ds(pl.multiple_of(t * GROUP, GROUP), GROUP)
        rows = pl.ds(pl.multiple_of(b * GROUP, GROUP), GROUP)
        gated = mbuf[0, here, :]
        for l in range(1, levels):
            gated += mbuf[l, here, :]
        gated = gated * gates[rows, :]
        total_sq = jnp.broadcast_to(jnp.sum(gated * gated, axis=1, keepdims=True), (GROUP, LANES))
        product = jnp.dot((gated * ogain[...]).astype(bf16), owbuf[...], preferred_element_type=f32)
        for j in range(per):
            osend[b, j, :, :out_cols] = product[j * out_rows : (j + 1) * out_rows]
            osend[b, j, :, out_cols:] = total_sq[j * out_rows : (j + 1) * out_rows]
        for j in range(per):
            @pl.when(b * per + j != me_h)
            def _():
                send(osend.at[b, j], orecv.at[me_h], sent, o_recv, (b * per + j, me_l))

    total = osend[block, me_j]
    arrived(orecv.at[pl.ds(0, heads - 1)], o_recv)
    for o in range(1, heads):
        total += orecv[lax.rem(me_h + heads - o, heads)]
    mean = total[:, out_cols : out_cols + 1] / (heads * val_dim)
    out[...] = total[:, :out_cols] * lax.rsqrt(mean + 1e-05)
    arrived(xbuf.at[pl.ds(0, heads - 1)], sent)
    arrived(kx.at[pl.ds(0, levels - 1), 0], sent)
    arrived(kx.at[pl.ds(0, levels - 1), pl.ds(0, heads - 1)], sent)
    arrived(tbuf.at[pl.ds(0, levels - 1)], sent)
    arrived(qbuf.at[pl.ds(0, levels - 1)], sent)
    arrived(gates.at[pl.ds(0, seqs - owned)], sent)
    arrived(mbuf.at[pl.ds(0, levels - 1)], sent)
    arrived(orecv.at[pl.ds(0, heads - 1)], sent)


def body(features, in_gain, in_weight, level_bias, states, positions, out_gain, out_weight):
    heads, levels = lax.axis_size("head"), lax.axis_size("level")
    seqs, fw = features.shape
    width, cols = in_weight.shape
    _, head_here, level_here, key_dim, val_dim = states.shape
    level_total = level_bias.shape[1]
    assert seqs // levels <= GROUP and head_here == 1 and key_dim == LANES and val_dim == LANES
    out_cols = out_weight.shape[1]
    flipped = fw % LANES == 0
    slots = LANES // (1 << level_total.bit_length())
    owned, out_rows, groups = seqs // levels, seqs // heads, seqs // GROUP
    f32, bf16 = jnp.float32, jnp.bfloat16
    vmem, anyspace = pl.BlockSpec(memory_space=pltpu.VMEM), pl.BlockSpec(memory_space=pl.ANY)
    dma = pltpu.SemaphoreType.DMA
    return pl.pallas_call(
        functools.partial(kernel, heads, levels, in_gain.shape[0], (key_dim, val_dim, level_total, level_here)),
        out_shape=pltpu.VMEM((out_rows, out_cols), f32),
        in_specs=[anyspace] * 8,
        out_specs=vmem,
        scratch_shapes=[
            pltpu.VMEM((heads * levels, fw), f32),
            pltpu.VMEM(level_bias.shape, f32),
            pltpu.VMEM((1, seqs), jnp.int32),
            pltpu.VMEM((1, val_dim), f32),
            pltpu.VMEM((heads, seqs, fw), f32),
            pltpu.VMEM((cols, width) if flipped else (width, cols), bf16),
            pltpu.VMEM((seqs, level_here * key_dim, val_dim), bf16),
            pltpu.VMEM(out_weight.shape, bf16),
            pltpu.VMEM((seqs, LANES), f32),
            pltpu.VMEM((levels, seqs // slots, LANES), f32),
            pltpu.VMEM((levels, seqs, key_dim), f32),
            pltpu.VMEM((seqs, key_dim), f32),
            pltpu.VMEM((levels, heads, owned, fw), f32),
            pltpu.VMEM((seqs, val_dim), f32),
            pltpu.VMEM((owned, 3 * LANES), f32),
            pltpu.VMEM((owned, fw), f32),
            pltpu.VMEM((owned, val_dim), f32),
            pltpu.VMEM((seqs, level_here * key_dim), f32),
            pltpu.VMEM((seqs, 2 * LANES), f32),
            pltpu.VMEM((levels, seqs, val_dim), f32),
            pltpu.VMEM((groups, heads // groups, out_rows, out_cols + LANES), f32),
            pltpu.VMEM((heads, out_rows, out_cols + LANES), f32),
            pltpu.VMEM((1, LANES), f32),
            pltpu.SemaphoreType.REGULAR,
            dma((4,)), *[dma(())] * 5, dma((heads,)), dma((levels,)), dma(()),
            dma(()), dma((groups,)), dma((levels,)), dma((groups,)), dma(()),
        ],
        compiler_params=pltpu.CompilerParams(collective_id=0, has_side_effects=True),
    )(
        features,
        in_gain.reshape(heads * levels, fw),
        in_weight.T if flipped else in_weight,
        level_bias,
        states.reshape(seqs, level_here * key_dim, val_dim),
        positions.reshape(1, seqs),
        out_gain.reshape(1, val_dim),
        out_weight,
    )


def solution(mesh):
    in_specs = (
        P(None, ("head", "level")),
        P(),
        P(None, "head"),
        P("head", None),
        P(None, "head", "level", None, None),
        P(),
        P("head"),
        P("head", "level"),
    )
    out_specs = P("head", "level")
    return jax.shard_map(body, mesh=mesh, in_specs=in_specs, out_specs=out_specs, check_vma=False)
```

```python
import functools

import jax
import jax.numpy as jnp
from jax import lax
from jax.experimental import pallas as pl
from jax.experimental.pallas import tpu as pltpu
from jax.sharding import PartitionSpec as P

LANES = 128
GROUP = 16
POSITION_BITS = 18


def send(src, dst, send_sem, recv_sem, target):
    c = pltpu.make_async_remote_copy(
        src_ref=src,
        dst_ref=dst,
        send_sem=send_sem,
        recv_sem=recv_sem,
        device_id=target,
        device_id_type=pl.DeviceIdType.MESH,
    )
    c.start()


def arrived(like, sem):
    pltpu.make_async_copy(like, like, sem).wait()


def exclusive_or(a, b, count):
    result, bit = 0, 1
    while bit < count:
        result = result + bit * lax.rem(a // bit + b // bit, 2)
        bit *= 2
    return result


def kernel(
    heads, levels, width, dims,
    feat, gain_any, inw, bias_any, states, pos_any, ogain_any, outw, out,
    gain, bias, pos, ogain, xbuf, wbuf, sbuf, owbuf, tailbuf, tbuf, qbuf, qtmp, kx, gates, restbuf, sqbuf, ownbuf,
    wexp, scales, mbuf, osend, orecv, qsend, qrow, biasbuf,
    z_sem, x_sem, w_sem, s_sem, ow_sem, sent, f_recv, kx_recv, k2_recv,
    t_recv, q_recv, g_recv, m_recv, o_recv, r_recv,
):
    key_dim, val_dim, level_total, level_here = dims
    seqs, fw = feat.shape
    flipped = fw % LANES == 0
    owned = seqs // levels
    out_rows = seqs // heads
    out_cols = outw.shape[1]
    me_h, me_l = lax.axis_index("head"), lax.axis_index("level")
    slot = 1 << level_total.bit_length()
    slots = LANES // slot
    packed = seqs // slots
    groups = seqs // GROUP
    per = heads // groups
    block, me_j = me_h // per, lax.rem(me_h, per)
    order = [exclusive_or(block, groups - 1 - t, groups) for t in range(groups)]
    my_block = me_l * owned // GROUP
    my_t = groups - 1 - exclusive_or(block, my_block, groups)
    own_rows = pl.ds(pl.multiple_of(my_t * GROUP + lax.rem(me_l * owned, GROUP), owned), owned)
    mine = pl.ds(pl.multiple_of(me_l * owned, owned), owned)

    def by_level(choice):
        value = jnp.int32(choice(0))
        for l in range(1, levels):
            value = jnp.where(me_l == l, choice(l), value)
        return value

    peers = [
        by_level(lambda me: sorted((p for p in range(levels) if p != me), key=lambda p: (-abs(p - me), p))[s])
        for s in range(levels - 1)]
    tail0 = 2 * key_dim + 2 * val_dim
    f32, bf16 = jnp.float32, jnp.bfloat16

    def group_rows(t):
        return pl.ds(pl.multiple_of(order[t] * GROUP, GROUP), GROUP)

    def rows_of_group(ref, t, first=0, last=LANES):
        return ref[group_rows(t), first:last]

    x_copy = pltpu.make_async_copy(feat, xbuf.at[me_h], x_sem)
    x_copy.start()

    def tell(sem, h, l):
        pl.semaphore_signal(sem, inc=1, device_id=(h, l), device_id_type=pl.DeviceIdType.MESH)

    core = lax.rem(me_h, 2)
    buddy = me_h + 1 - 2 * core
    barrier = pltpu.get_barrier_semaphore()
    pl.loop(me_l + 1, levels)(lambda l: tell(barrier, me_h, l))
    for o in range(1, heads):
        tell(barrier, lax.rem(me_h + o, heads), me_l)
    smalls = [
        pltpu.make_async_copy(a, b, w_sem)
        for a, b in ((gain_any, gain), (bias_any, bias), (pos_any, pos), (ogain_any, ogain))]
    for c in smalls:
        c.start()
    if flipped:
        for l in range(levels):
            for h in range(heads):
                pltpu.make_async_copy(
                    inw.at[:, pl.ds((h * levels + l) * fw, fw)], wbuf.at[:, pl.ds((l * heads + h) * fw, fw)], w_sem).start()
    else:
        pltpu.make_async_copy(inw, wbuf, w_sem).start()
    pl.semaphore_wait(barrier, heads - 1 + me_l)
    pl.loop(0, me_l)(lambda l: tell(z_sem, me_h, l))

    x_copy.wait()

    def feature_send(source, target):
        send(xbuf.at[source], xbuf.at[source], sent, f_recv.at[source], (target, me_l))

    def feature_wait(source):
        arrived(xbuf.at[source], f_recv.at[source])

    chips = heads // 2
    mirror_chip = chips - 1 - me_h // 2
    skip = lax.rem(me_h // 2 - mirror_chip + chips, chips)
    mirror = 2 * mirror_chip + core
    direct = []
    for j in range(1, chips - 1):
        near = 2 * lax.rem(mirror_chip + j + (j + chips - skip) // chips, chips)
        direct += [near + core, near + 1 - core]
    feature_send(me_h, mirror)
    for peer in direct:
        feature_send(me_h, peer)
    feature_send(me_h, buddy)

    def rows_send(l):
        theirs = pl.ds(pl.multiple_of(l * owned, owned), owned)
        send(xbuf.at[me_h, theirs], kx.at[me_l, me_h], sent, kx_recv.at[me_l], (me_h, l))

    pl.loop(0, me_l)(rows_send)
    possible = min(level_total, POSITION_BITS + 1)
    counts = sorted({min(max(possible - l * level_here, 0), level_here) for l in range(levels)})
    count = jnp.clip(possible - me_l * level_here, 0, level_here)

    def state_start(t, n):
        part = (group_rows(t), pl.ds(0, n * key_dim))
        pltpu.make_async_copy(states.at[part], sbuf.at[part], s_sem).start()

    for n in counts:
        @pl.when(jnp.logical_and(count == n, n > 0))
        def _():
            for t in range(groups):
                state_start(t, n)

    for c in smalls:
        c.wait()
    arrived(wbuf, w_sem)

    def weight(first, last, h, l):
        if flipped:
            return wbuf[first:last, pl.ds(pl.multiple_of((l * heads + h) * fw, fw), fw)]
        return wbuf[pl.ds(pl.multiple_of((h * levels + l) * fw, fw), fw), first:last]

    def project(x, w):
        return lax.dot_general(x, w, (((1,), (1 if flipped else 0,)), ((), ())), preferred_element_type=f32)

    query = jnp.zeros((seqs, key_dim), f32)
    tail = jnp.zeros((seqs, level_total), f32)
    squares = jnp.zeros((seqs, fw), f32)
    arrivals = [me_h, buddy, mirror] + direct + [2 * mirror_chip + 1 - core]
    for i, src in enumerate(arrivals):
        if i == len(arrivals) - 2:
            @pl.when(me_l < levels - 1)
            def _():
                pl.semaphore_wait(z_sem, levels - 1 - me_l)

            pl.loop(me_l + 1, levels)(rows_send)
        if i:
            feature_wait(src)
        if i == 2:
            feature_send(mirror, buddy)
        x = xbuf[src]
        index = src * levels + me_l
        scaled = (x * gain[pl.ds(index, 1), :]).astype(bf16)
        query += project(scaled, weight(0, key_dim, src, me_l))
        tail += project(scaled, weight(tail0, tail0 + level_total, src, me_l))
        squares += x * x
    squares = jnp.sum(squares, axis=1, keepdims=True)

    tailbuf[:, :level_total] = tail
    lane = lax.broadcasted_iota(jnp.int32, (seqs, LANES), 1)
    tail = jnp.where(lane < level_total, tailbuf[...], 0.0)
    tail = jnp.where(lane == level_total, squares, tail)
    pack = tail[:packed]
    for c in range(1, slots):
        pack += pltpu.roll(tail[c * packed : (c + 1) * packed], slot * c, 1)
    tbuf[me_l] = pack
    qtmp[...] = query
    for t in range(groups):
        qbuf[me_l, t * GROUP : (t + 1) * GROUP] = rows_of_group(qtmp, t)
    for peer in peers:
        send(tbuf.at[me_l], tbuf.at[me_l], sent, t_recv, (me_h, peer))
    for t in range(groups):
        part = qbuf.at[me_l, pl.ds(t * GROUP, GROUP)]
        for peer in peers:
            send(part, part, sent, q_recv.at[t], (me_h, peer))

    ow_copy = pltpu.make_async_copy(outw, owbuf, ow_sem)
    ow_copy.start()

    biasbuf[:, :level_total] = bias[...]
    row = lax.broadcasted_iota(jnp.int32, (seqs, seqs), 0)
    col = lax.broadcasted_iota(jnp.int32, (seqs, seqs), 1)
    pos_f = jnp.broadcast_to(pos[...], (seqs, seqs)).astype(f32)
    pos_col = jnp.sum(jnp.where(row == col, pos_f, 0.0), axis=1, keepdims=True).astype(jnp.int32)
    shift = jnp.clip(lane - 1, 0, 31)
    bits = jnp.bitwise_and(jnp.right_shift(jnp.broadcast_to(pos_col, lane.shape), shift), 1)
    occupied = jnp.logical_and(lane < level_total, jnp.logical_or(lane == 0, bits == 1))

    def piece(l, rows_of):
        total = jnp.zeros((owned, fw), f32)
        if flipped:
            scaled = []
            for h in range(heads):
                x = rows_of(h)
                scaled.append((x * gain[pl.ds(h * levels + l, 1), :]).astype(bf16))
                total += x * x
            at = pl.ds(pl.multiple_of(l * heads * fw, heads * fw), heads * fw)
            return project(jnp.concatenate(scaled, axis=1), wbuf[key_dim:tail0, at]), total

        def step(h, carry):
            rest, total = carry
            x = rows_of(h)
            scaled = (x * gain[pl.ds(h * levels + l, 1), :]).astype(bf16)
            return rest + project(scaled, weight(key_dim, tail0, h, l)), total + x * x

        return lax.fori_loop(0, heads, step, (jnp.zeros((owned, tail0 - key_dim), f32), total))

    for s in range(levels - 1):
        l = by_level(lambda me: sorted((p for p in range(levels) if p != me), key=lambda p: (abs(p - me), p))[s])
        arrived(kx.at[0, 0], kx_recv.at[l])
        part = kx.at[l, me_h]
        for target in [mirror, 2 * mirror_chip + 1 - core] + direct + [buddy]:
            send(part, part, sent, k2_recv, (target, me_l))

    restbuf[...], sqbuf[...] = piece(me_l, lambda h: xbuf[h, mine, :])

    arrived(tbuf.at[pl.ds(0, levels - 1)], t_recv)
    pack = tbuf[0]
    for l in range(1, levels):
        pack += tbuf[l]
    parts = [pack] + [pltpu.roll(pack, LANES - slot * c, 1) for c in range(1, slots)]
    tail = jnp.concatenate(parts, axis=0)
    row_scale = lax.rsqrt(tail[:, level_total : level_total + 1] / width + 1e-06)
    logits = tail * row_scale + biasbuf[...]
    peak = jnp.max(jnp.where(occupied, logits, -1e30), axis=1, keepdims=True)
    weights = jnp.where(occupied, jnp.exp(logits - peak), 0.0)
    weights = weights / jnp.sum(weights, axis=1, keepdims=True)
    local = pltpu.roll(weights, lax.rem(LANES - me_l * level_here, LANES), 1)
    for j in range(level_here):
        wexp[:, j * key_dim : (j + 1) * key_dim] = jnp.broadcast_to(local[:, j : j + 1], (seqs, key_dim))
    scales[:, :LANES] = jnp.broadcast_to(row_scale, weights.shape)
    scales[:, LANES:] = jnp.broadcast_to(weights[:, :1], weights.shape)

    def query_wait(t):
        arrived(qbuf.at[pl.ds(0, levels - 1), pl.ds(0, GROUP)], q_recv.at[t])

    def own_and_gate(last):
        rest, squares = restbuf[...], sqbuf[...]
        arrived(kx.at[pl.ds(0, levels - 1), pl.ds(0, heads - 1)], k2_recv)
        for l in peers:
            more = piece(l, lambda h: kx[l, h])
            rest, squares = rest + more[0], squares + more[1]
        rest = rest * lax.rsqrt(jnp.sum(squares, axis=1, keepdims=True) / width + 1e-06)
        key, value, gate = [rest[:, j * key_dim : (j + 1) * key_dim] for j in range(3)]
        gates[mine, :] = gate * jax.nn.sigmoid(gate)
        for peer in peers:
            send(gates.at[mine], gates.at[mine], sent, g_recv.at[me_l], (me_h, peer))
        if last:
            query_wait(groups - 1)
        query = qbuf[0, own_rows, :]
        for l in range(1, levels):
            query += qbuf[l, own_rows, :]
        query = query * scales[mine, :LANES]
        own = jnp.sum(query * key, axis=1, keepdims=True) * key_dim ** (-0.5) * value
        ownbuf[...] = scales[mine, LANES:] * own

    def own_send():
        mbuf[me_l, own_rows, :] += ownbuf[...]
        reads_send(my_t)

    seq_in = lax.broadcasted_iota(jnp.int32, (GROUP, val_dim), 0)
    def reads_send(t):
        part = mbuf.at[me_l, pl.ds(pl.multiple_of(t * GROUP, GROUP), GROUP)]
        for peer in peers:
            send(part, part, sent, m_recv.at[t], (me_h, peer))

    def read_group(t, n):
        here = pl.ds(t * GROUP, GROUP)
        reads = jnp.zeros((GROUP, val_dim), f32)
        if n:
            query = qbuf[0, here, :]
            for l in range(1, levels):
                query += qbuf[l, here, :]
            low = (query * rows_of_group(scales, t)).astype(bf16).astype(f32)
            left = jnp.concatenate(
                [(low * rows_of_group(wexp, t, j * key_dim, (j + 1) * key_dim)).astype(bf16) for j in range(n)], axis=1)
            for i in range(GROUP):
                seq = order[t] * GROUP + i
                got = jnp.dot(left, sbuf[seq, : n * key_dim, :], preferred_element_type=f32)
                reads = jnp.where(seq_in == i, got, reads)
        mbuf[me_l, here, :] = reads

        @pl.when(order[t] != my_block)
        def _():
            reads_send(t)

    for n in counts:
        @pl.when(count == n)
        def _():
            if n:
                arrived(sbuf.at[:, pl.ds(0, n * key_dim)], s_sem)
            for t in range(groups - 1):
                query_wait(t)
                read_group(t, n)
            if n < level_here:
                query_wait(groups - 1)
                read_group(groups - 1, n)
            own_and_gate(n == level_here)
            if n < level_here:
                own_send()
            else:
                pl.when(my_t < groups - 1)(own_send)
                read_group(groups - 1, n)
                pl.when(my_t == groups - 1)(own_send)

    def nearest(l, own, s):
        return sorted(range(groups), key=lambda b: (b == own, abs((2 * b + 1) * levels - (2 * l + 1) * groups), b))[s]

    ow_copy.wait()
    lane_of = lax.broadcasted_iota(jnp.int32, (GROUP, LANES), 1)
    row_of = lax.broadcasted_iota(jnp.int32, (GROUP, LANES), 0)
    for s in range(groups):
        b = by_level(lambda l: nearest(l, 0, s))
        for own in range(1, groups):
            b = jnp.where(block == own, by_level(lambda l: nearest(l, own, s)), b)
        t = groups - 1 - exclusive_or(block, b, groups)
        for o in range(GROUP // owned):
            owner = b * (GROUP // owned) + o

            @pl.when(owner != me_l)
            def _():
                arrived(gates.at[pl.ds(0, owned)], g_recv.at[owner])

        arrived(mbuf.at[pl.ds(0, levels - 1), pl.ds(0, GROUP)], m_recv.at[t])
        here = pl.ds(pl.multiple_of(t * GROUP, GROUP), GROUP)
        rows = pl.ds(pl.multiple_of(b * GROUP, GROUP), GROUP)
        gated = mbuf[0, here, :]
        for l in range(1, levels):
            gated += mbuf[l, here, :]
        gated = gated * gates[rows, :]
        total_sq = jnp.broadcast_to(jnp.sum(gated * gated, axis=1, keepdims=True), (GROUP, LANES))
        qsend[b] = jnp.sum(jnp.where(row_of == lane_of, total_sq, 0.0), axis=0, keepdims=True)
        product = jnp.dot((gated * ogain[...]).astype(bf16), owbuf[...], preferred_element_type=f32)
        for j in range(per):
            osend[b, j] = product[j * out_rows : (j + 1) * out_rows]
        for j in range(per):
            @pl.when(b * per + j != me_h)
            def _():
                send(qsend.at[b], qrow.at[me_h], sent, r_recv, (b * per + j, me_l))
                send(osend.at[b, j], orecv.at[me_h], sent, o_recv, (b * per + j, me_l))

    total = osend[block, me_j]
    square = qsend[block]
    arrived(qrow.at[pl.ds(0, heads - 1)], r_recv)
    for o in range(1, heads):
        square += qrow[lax.rem(me_h + heads - o, heads)]
    lane_of = lax.broadcasted_iota(jnp.int32, (out_rows, LANES), 1)
    row_of = lax.broadcasted_iota(jnp.int32, (out_rows, LANES), 0) + me_j * out_rows
    square = jnp.where(row_of == lane_of, jnp.broadcast_to(square, (out_rows, LANES)), 0.0)
    factor = lax.rsqrt(jnp.sum(square, axis=1, keepdims=True) / (heads * val_dim) + 1e-05)
    arrived(orecv.at[pl.ds(0, heads - 1)], o_recv)
    for o in range(1, heads):
        total += orecv[lax.rem(me_h + heads - o, heads)]
    out[...] = total * factor
    arrived(xbuf.at[pl.ds(0, heads - 1)], sent)
    arrived(kx.at[pl.ds(0, levels - 1), 0], sent)
    arrived(kx.at[pl.ds(0, levels - 1), pl.ds(0, heads - 1)], sent)
    arrived(tbuf.at[pl.ds(0, levels - 1)], sent)
    arrived(qbuf.at[pl.ds(0, levels - 1)], sent)
    arrived(gates.at[pl.ds(0, seqs - owned)], sent)
    arrived(mbuf.at[pl.ds(0, levels - 1)], sent)
    arrived(orecv.at[pl.ds(0, heads - 1)], sent)
    arrived(qrow.at[pl.ds(0, heads - 1)], sent)


def body(features, in_gain, in_weight, level_bias, states, positions, out_gain, out_weight):
    heads, levels = lax.axis_size("head"), lax.axis_size("level")
    seqs, fw = features.shape
    width, cols = in_weight.shape
    _, head_here, level_here, key_dim, val_dim = states.shape
    level_total = level_bias.shape[1]
    assert seqs // levels <= GROUP and head_here == 1 and key_dim == LANES and val_dim == LANES
    out_cols = out_weight.shape[1]
    flipped = fw % LANES == 0
    slots = LANES // (1 << level_total.bit_length())
    owned, out_rows, groups = seqs // levels, seqs // heads, seqs // GROUP
    f32, bf16 = jnp.float32, jnp.bfloat16
    vmem, anyspace = pl.BlockSpec(memory_space=pltpu.VMEM), pl.BlockSpec(memory_space=pl.ANY)
    dma = pltpu.SemaphoreType.DMA
    return pl.pallas_call(
        functools.partial(kernel, heads, levels, in_gain.shape[0], (key_dim, val_dim, level_total, level_here)),
        out_shape=pltpu.VMEM((out_rows, out_cols), f32),
        in_specs=[anyspace] * 8,
        out_specs=vmem,
        scratch_shapes=[
            pltpu.VMEM((heads * levels, fw), f32),
            pltpu.VMEM(level_bias.shape, f32),
            pltpu.VMEM((1, seqs), jnp.int32),
            pltpu.VMEM((1, val_dim), f32),
            pltpu.VMEM((heads, seqs, fw), f32),
            pltpu.VMEM((cols, width) if flipped else (width, cols), bf16),
            pltpu.VMEM((seqs, level_here * key_dim, val_dim), bf16),
            pltpu.VMEM(out_weight.shape, bf16),
            pltpu.VMEM((seqs, LANES), f32),
            pltpu.VMEM((levels, seqs // slots, LANES), f32),
            pltpu.VMEM((levels, seqs, key_dim), f32),
            pltpu.VMEM((seqs, key_dim), f32),
            pltpu.VMEM((levels, heads, owned, fw), f32),
            pltpu.VMEM((seqs, val_dim), f32),
            pltpu.VMEM((owned, 3 * LANES), f32),
            pltpu.VMEM((owned, fw), f32),
            pltpu.VMEM((owned, val_dim), f32),
            pltpu.VMEM((seqs, level_here * key_dim), f32),
            pltpu.VMEM((seqs, 2 * LANES), f32),
            pltpu.VMEM((levels, seqs, val_dim), f32),
            pltpu.VMEM((groups, heads // groups, out_rows, out_cols), f32),
            pltpu.VMEM((heads, out_rows, out_cols), f32),
            pltpu.VMEM((groups, 1, LANES), f32),
            pltpu.VMEM((heads, 1, LANES), f32),
            pltpu.VMEM((1, LANES), f32),
            pltpu.SemaphoreType.REGULAR,
            *[dma(())] * 5, dma((heads,)), dma((levels,)), dma(()),
            dma(()), dma((groups,)), dma((levels,)), dma((groups,)), dma(()), dma(()),
        ],
        compiler_params=pltpu.CompilerParams(collective_id=0, has_side_effects=True),
    )(
        features,
        in_gain.reshape(heads * levels, fw),
        in_weight.T if flipped else in_weight,
        level_bias,
        states.reshape(seqs, level_here * key_dim, val_dim),
        positions.reshape(1, seqs),
        out_gain.reshape(1, val_dim),
        out_weight,
    )


def solution(mesh):
    in_specs = (
        P(None, ("head", "level")),
        P(),
        P(None, "head"),
        P("head", None),
        P(None, "head", "level", None, None),
        P(),
        P("head"),
        P("head", "level"),
    )
    out_specs = P("head", "level")
    return jax.shard_map(body, mesh=mesh, in_specs=in_specs, out_specs=out_specs, check_vma=False)
```

```python
import functools

import jax
import jax.numpy as jnp
from jax import lax
from jax.experimental import pallas as pl
from jax.experimental.pallas import tpu as pltpu
from jax.sharding import PartitionSpec as P

LANES = 128
GROUP = 16
POSITION_BITS = 18


def send(src, dst, send_sem, recv_sem, target):
    c = pltpu.make_async_remote_copy(
        src_ref=src,
        dst_ref=dst,
        send_sem=send_sem,
        recv_sem=recv_sem,
        device_id=target,
        device_id_type=pl.DeviceIdType.MESH,
    )
    c.start()


def arrived(like, sem):
    pltpu.make_async_copy(like, like, sem).wait()


def exclusive_or(a, b, count):
    result, bit = 0, 1
    while bit < count:
        result = result + bit * lax.rem(a // bit + b // bit, 2)
        bit *= 2
    return result


def kernel(
    heads, levels, width, dims,
    feat, gain_any, inw, bias_any, states, pos_any, ogain_any, outw, out,
    gain, bias, pos, ogain, xbuf, wbuf, sbuf, owbuf, tailbuf, tbuf, qbuf, qtmp, kx, gates, restbuf, sqbuf, ownbuf,
    wexp, scales, mbuf, osend, orecv, qsend, qrow, biasbuf,
    z_sem, x_sem, w_sem, s_sem, ow_sem, sent, f_recv, kx_recv, k2_recv,
    t_recv, q_recv, g_recv, m_recv, o_recv, r_recv,
):
    key_dim, val_dim, level_total, level_here = dims
    seqs, fw = feat.shape
    flipped = fw % LANES == 0
    owned = seqs // levels
    out_rows = seqs // heads
    out_cols = outw.shape[1]
    me_h, me_l = lax.axis_index("head"), lax.axis_index("level")
    slot = 1 << level_total.bit_length()
    slots = LANES // slot
    packed = seqs // slots
    groups = seqs // GROUP
    per = heads // groups
    block, me_j = me_h // per, lax.rem(me_h, per)
    order = [exclusive_or(block, groups - 1 - t, groups) for t in range(groups)]
    my_block = me_l * owned // GROUP
    my_t = groups - 1 - exclusive_or(block, my_block, groups)
    own_rows = pl.ds(pl.multiple_of(my_t * GROUP + lax.rem(me_l * owned, GROUP), owned), owned)
    mine = pl.ds(pl.multiple_of(me_l * owned, owned), owned)

    def by_level(choice):
        value = jnp.int32(choice(0))
        for l in range(1, levels):
            value = jnp.where(me_l == l, choice(l), value)
        return value

    peers = [
        by_level(lambda me: sorted((p for p in range(levels) if p != me), key=lambda p: (-abs(p - me), p))[s])
        for s in range(levels - 1)]
    tail0 = 2 * key_dim + 2 * val_dim
    f32, bf16 = jnp.float32, jnp.bfloat16

    def group_rows(t):
        return pl.ds(pl.multiple_of(order[t] * GROUP, GROUP), GROUP)

    def rows_of_group(ref, t, first=0, last=LANES):
        return ref[group_rows(t), first:last]

    x_copy = pltpu.make_async_copy(feat, xbuf.at[me_h], x_sem)
    x_copy.start()

    def tell(sem, h, l):
        pl.semaphore_signal(sem, inc=1, device_id=(h, l), device_id_type=pl.DeviceIdType.MESH)

    core = lax.rem(me_h, 2)
    buddy = me_h + 1 - 2 * core
    barrier = pltpu.get_barrier_semaphore()
    pl.loop(me_l + 1, levels)(lambda l: tell(barrier, me_h, l))
    for o in range(1, heads):
        tell(barrier, lax.rem(me_h + o, heads), me_l)
    smalls = [
        pltpu.make_async_copy(a, b, w_sem)
        for a, b in ((gain_any, gain), (bias_any, bias), (pos_any, pos), (ogain_any, ogain))]
    for c in smalls:
        c.start()
    if flipped:
        for l in range(levels):
            for h in range(heads):
                pltpu.make_async_copy(
                    inw.at[:, pl.ds((h * levels + l) * fw, fw)], wbuf.at[:, pl.ds((l * heads + h) * fw, fw)], w_sem).start()
    else:
        pltpu.make_async_copy(inw, wbuf, w_sem).start()
    pl.semaphore_wait(barrier, heads - 1 + me_l)
    pl.loop(0, me_l)(lambda l: tell(z_sem, me_h, l))

    x_copy.wait()

    def feature_send(source, target):
        send(xbuf.at[source], xbuf.at[source], sent, f_recv.at[source], (target, me_l))

    def feature_wait(source):
        arrived(xbuf.at[source], f_recv.at[source])

    chips = heads // 2
    mirror_chip = chips - 1 - me_h // 2
    skip = lax.rem(me_h // 2 - mirror_chip + chips, chips)
    mirror = 2 * mirror_chip + core
    direct = []
    for j in range(1, chips - 1):
        near = 2 * lax.rem(mirror_chip + j + (j + chips - skip) // chips, chips)
        direct += [near + core, near + 1 - core]
    feature_send(me_h, mirror)
    for peer in direct:
        feature_send(me_h, peer)
    feature_send(me_h, buddy)

    def rows_send(l):
        theirs = pl.ds(pl.multiple_of(l * owned, owned), owned)
        send(xbuf.at[me_h, theirs], kx.at[me_l, me_h], sent, kx_recv, (me_h, l))

    pl.loop(0, me_l)(rows_send)
    possible = min(level_total, POSITION_BITS + 1)
    counts = sorted({min(max(possible - l * level_here, 0), level_here) for l in range(levels)})
    count = jnp.clip(possible - me_l * level_here, 0, level_here)

    def state_start(t, n):
        part = (group_rows(t), pl.ds(0, n * key_dim))
        pltpu.make_async_copy(states.at[part], sbuf.at[part], s_sem).start()

    for n in counts:
        @pl.when(jnp.logical_and(count == n, n > 0))
        def _():
            for t in range(groups):
                state_start(t, n)

    for c in smalls:
        c.wait()
    arrived(wbuf, w_sem)

    def weight(first, last, h, l):
        if flipped:
            return wbuf[first:last, pl.ds(pl.multiple_of((l * heads + h) * fw, fw), fw)]
        return wbuf[pl.ds(pl.multiple_of((h * levels + l) * fw, fw), fw), first:last]

    def project(x, w):
        return lax.dot_general(x, w, (((1,), (1 if flipped else 0,)), ((), ())), preferred_element_type=f32)

    query = jnp.zeros((seqs, key_dim), f32)
    tail = jnp.zeros((seqs, level_total), f32)
    squares = jnp.zeros((seqs, fw), f32)
    arrivals = [me_h, buddy, mirror] + direct + [2 * mirror_chip + 1 - core]
    for i, src in enumerate(arrivals):
        if i == len(arrivals) - 2:
            @pl.when(me_l < levels - 1)
            def _():
                pl.semaphore_wait(z_sem, levels - 1 - me_l)

            pl.loop(0, levels - 1 - me_l)(lambda s: rows_send(levels - 1 - s))
        if i:
            feature_wait(src)
        if i == 2:
            feature_send(mirror, buddy)
        x = xbuf[src]
        index = src * levels + me_l
        scaled = (x * gain[pl.ds(index, 1), :]).astype(bf16)
        query += project(scaled, weight(0, key_dim, src, me_l))
        tail += project(scaled, weight(tail0, tail0 + level_total, src, me_l))
        squares += x * x
    squares = jnp.sum(squares, axis=1, keepdims=True)

    tailbuf[:, :level_total] = tail
    lane = lax.broadcasted_iota(jnp.int32, (seqs, LANES), 1)
    tail = jnp.where(lane < level_total, tailbuf[...], 0.0)
    tail = jnp.where(lane == level_total, squares, tail)
    pack = tail[:packed]
    for c in range(1, slots):
        pack += pltpu.roll(tail[c * packed : (c + 1) * packed], slot * c, 1)
    tbuf[me_l] = pack
    qtmp[...] = query
    for t in range(groups):
        qbuf[me_l, t * GROUP : (t + 1) * GROUP] = rows_of_group(qtmp, t)
    for peer in peers:
        send(tbuf.at[me_l], tbuf.at[me_l], sent, t_recv, (me_h, peer))
    for t in range(groups):
        part = qbuf.at[me_l, pl.ds(t * GROUP, GROUP)]
        for peer in peers:
            send(part, part, sent, q_recv.at[t], (me_h, peer))

    ow_copy = pltpu.make_async_copy(outw, owbuf, ow_sem)
    ow_copy.start()

    biasbuf[:, :level_total] = bias[...]
    row = lax.broadcasted_iota(jnp.int32, (seqs, seqs), 0)
    col = lax.broadcasted_iota(jnp.int32, (seqs, seqs), 1)
    pos_f = jnp.broadcast_to(pos[...], (seqs, seqs)).astype(f32)
    pos_col = jnp.sum(jnp.where(row == col, pos_f, 0.0), axis=1, keepdims=True).astype(jnp.int32)
    shift = jnp.clip(lane - 1, 0, 31)
    bits = jnp.bitwise_and(jnp.right_shift(jnp.broadcast_to(pos_col, lane.shape), shift), 1)
    occupied = jnp.logical_and(lane < level_total, jnp.logical_or(lane == 0, bits == 1))

    def piece(l, rows_of):
        total = jnp.zeros((owned, fw), f32)
        if flipped:
            scaled = []
            for h in range(heads):
                x = rows_of(h)
                scaled.append((x * gain[pl.ds(h * levels + l, 1), :]).astype(bf16))
                total += x * x
            at = pl.ds(pl.multiple_of(l * heads * fw, heads * fw), heads * fw)
            return project(jnp.concatenate(scaled, axis=1), wbuf[key_dim:tail0, at]), total

        def step(h, carry):
            rest, total = carry
            x = rows_of(h)
            scaled = (x * gain[pl.ds(h * levels + l, 1), :]).astype(bf16)
            return rest + project(scaled, weight(key_dim, tail0, h, l)), total + x * x

        return lax.fori_loop(0, heads, step, (jnp.zeros((owned, tail0 - key_dim), f32), total))

    arrived(kx.at[pl.ds(0, levels - 1), 0], kx_recv)
    for l in peers:
        part = kx.at[l, me_h]
        for target in [mirror, 2 * mirror_chip + 1 - core] + direct + [buddy]:
            send(part, part, sent, k2_recv, (target, me_l))

    restbuf[...], sqbuf[...] = piece(me_l, lambda h: xbuf[h, mine, :])

    arrived(tbuf.at[pl.ds(0, levels - 1)], t_recv)
    pack = tbuf[0]
    for l in range(1, levels):
        pack += tbuf[l]
    parts = [pack] + [pltpu.roll(pack, LANES - slot * c, 1) for c in range(1, slots)]
    tail = jnp.concatenate(parts, axis=0)
    row_scale = lax.rsqrt(tail[:, level_total : level_total + 1] / width + 1e-06)
    logits = tail * row_scale + biasbuf[...]
    peak = jnp.max(jnp.where(occupied, logits, -1e30), axis=1, keepdims=True)
    weights = jnp.where(occupied, jnp.exp(logits - peak), 0.0)
    weights = weights / jnp.sum(weights, axis=1, keepdims=True)
    local = pltpu.roll(weights, lax.rem(LANES - me_l * level_here, LANES), 1)
    for j in range(level_here):
        wexp[:, j * key_dim : (j + 1) * key_dim] = jnp.broadcast_to(local[:, j : j + 1], (seqs, key_dim))
    scales[:, :LANES] = jnp.broadcast_to(row_scale, weights.shape)
    scales[:, LANES:] = jnp.broadcast_to(weights[:, :1], weights.shape)

    def query_wait(t):
        arrived(qbuf.at[pl.ds(0, levels - 1), pl.ds(0, GROUP)], q_recv.at[t])

    def own_and_gate(last):
        rest, squares = restbuf[...], sqbuf[...]
        arrived(kx.at[pl.ds(0, levels - 1), pl.ds(0, heads - 1)], k2_recv)
        for l in peers:
            more = piece(l, lambda h: kx[l, h])
            rest, squares = rest + more[0], squares + more[1]
        rest = rest * lax.rsqrt(jnp.sum(squares, axis=1, keepdims=True) / width + 1e-06)
        key, value, gate = [rest[:, j * key_dim : (j + 1) * key_dim] for j in range(3)]
        gates[mine, :] = gate * jax.nn.sigmoid(gate)
        for peer in peers:
            send(gates.at[mine], gates.at[mine], sent, g_recv.at[me_l], (me_h, peer))
        if last:
            query_wait(groups - 1)
        query = qbuf[0, own_rows, :]
        for l in range(1, levels):
            query += qbuf[l, own_rows, :]
        query = query * scales[mine, :LANES]
        own = jnp.sum(query * key, axis=1, keepdims=True) * key_dim ** (-0.5) * value
        ownbuf[...] = scales[mine, LANES:] * own

    def own_send():
        mbuf[me_l, own_rows, :] += ownbuf[...]
        reads_send(my_t)

    seq_in = lax.broadcasted_iota(jnp.int32, (GROUP, val_dim), 0)
    def reads_send(t):
        part = mbuf.at[me_l, pl.ds(pl.multiple_of(t * GROUP, GROUP), GROUP)]
        for peer in peers:
            send(part, part, sent, m_recv.at[t], (me_h, peer))

    def read_group(t, n):
        here = pl.ds(t * GROUP, GROUP)
        reads = jnp.zeros((GROUP, val_dim), f32)
        if n:
            query = qbuf[0, here, :]
            for l in range(1, levels):
                query += qbuf[l, here, :]
            low = (query * rows_of_group(scales, t)).astype(bf16).astype(f32)
            left = jnp.concatenate(
                [(low * rows_of_group(wexp, t, j * key_dim, (j + 1) * key_dim)).astype(bf16) for j in range(n)], axis=1)
            for i in range(GROUP):
                seq = order[t] * GROUP + i
                got = jnp.dot(left, sbuf[seq, : n * key_dim, :], preferred_element_type=f32)
                reads = jnp.where(seq_in == i, got, reads)
        mbuf[me_l, here, :] = reads

        @pl.when(order[t] != my_block)
        def _():
            reads_send(t)

    for n in counts:
        @pl.when(count == n)
        def _():
            if n:
                arrived(sbuf.at[:, pl.ds(0, n * key_dim)], s_sem)
            for t in range(groups - 1):
                query_wait(t)
                read_group(t, n)
            if n < level_here:
                query_wait(groups - 1)
                read_group(groups - 1, n)
            own_and_gate(n == level_here)
            if n < level_here:
                own_send()
            else:
                pl.when(my_t < groups - 1)(own_send)
                read_group(groups - 1, n)
                pl.when(my_t == groups - 1)(own_send)

    def nearest(l, own, s):
        return sorted(range(groups), key=lambda b: (b == own, abs((2 * b + 1) * levels - (2 * l + 1) * groups), b))[s]

    ow_copy.wait()
    lane_of = lax.broadcasted_iota(jnp.int32, (GROUP, LANES), 1)
    row_of = lax.broadcasted_iota(jnp.int32, (GROUP, LANES), 0)
    for s in range(groups):
        b = by_level(lambda l: nearest(l, 0, s))
        for own in range(1, groups):
            b = jnp.where(block == own, by_level(lambda l: nearest(l, own, s)), b)
        t = groups - 1 - exclusive_or(block, b, groups)
        for o in range(GROUP // owned):
            owner = b * (GROUP // owned) + o

            @pl.when(owner != me_l)
            def _():
                arrived(gates.at[pl.ds(0, owned)], g_recv.at[owner])

        arrived(mbuf.at[pl.ds(0, levels - 1), pl.ds(0, GROUP)], m_recv.at[t])
        here = pl.ds(pl.multiple_of(t * GROUP, GROUP), GROUP)
        rows = pl.ds(pl.multiple_of(b * GROUP, GROUP), GROUP)
        gated = mbuf[0, here, :]
        for l in range(1, levels):
            gated += mbuf[l, here, :]
        gated = gated * gates[rows, :]
        total_sq = jnp.broadcast_to(jnp.sum(gated * gated, axis=1, keepdims=True), (GROUP, LANES))
        qsend[b] = jnp.sum(jnp.where(row_of == lane_of, total_sq, 0.0), axis=0, keepdims=True)
        product = jnp.dot((gated * ogain[...]).astype(bf16), owbuf[...], preferred_element_type=f32)
        for j in range(per):
            osend[b, j] = product[j * out_rows : (j + 1) * out_rows]
        for j in range(per):
            @pl.when(b * per + j != me_h)
            def _():
                send(qsend.at[b], qrow.at[me_h], sent, r_recv, (b * per + j, me_l))
                send(osend.at[b, j], orecv.at[me_h], sent, o_recv, (b * per + j, me_l))

    total = osend[block, me_j]
    square = qsend[block]
    arrived(qrow.at[pl.ds(0, heads - 1)], r_recv)
    for o in range(1, heads):
        square += qrow[lax.rem(me_h + heads - o, heads)]
    lane_of = lax.broadcasted_iota(jnp.int32, (out_rows, LANES), 1)
    row_of = lax.broadcasted_iota(jnp.int32, (out_rows, LANES), 0) + me_j * out_rows
    square = jnp.where(row_of == lane_of, jnp.broadcast_to(square, (out_rows, LANES)), 0.0)
    factor = lax.rsqrt(jnp.sum(square, axis=1, keepdims=True) / (heads * val_dim) + 1e-05)
    arrived(orecv.at[pl.ds(0, heads - 1)], o_recv)
    for o in range(1, heads):
        total += orecv[lax.rem(me_h + heads - o, heads)]
    out[...] = total * factor
    arrived(xbuf.at[pl.ds(0, heads - 1)], sent)
    arrived(kx.at[pl.ds(0, levels - 1), 0], sent)
    arrived(kx.at[pl.ds(0, levels - 1), pl.ds(0, heads - 1)], sent)
    arrived(tbuf.at[pl.ds(0, levels - 1)], sent)
    arrived(qbuf.at[pl.ds(0, levels - 1)], sent)
    arrived(gates.at[pl.ds(0, seqs - owned)], sent)
    arrived(mbuf.at[pl.ds(0, levels - 1)], sent)
    arrived(orecv.at[pl.ds(0, heads - 1)], sent)
    arrived(qrow.at[pl.ds(0, heads - 1)], sent)


def body(features, in_gain, in_weight, level_bias, states, positions, out_gain, out_weight):
    heads, levels = lax.axis_size("head"), lax.axis_size("level")
    seqs, fw = features.shape
    width, cols = in_weight.shape
    _, head_here, level_here, key_dim, val_dim = states.shape
    level_total = level_bias.shape[1]
    assert seqs // levels <= GROUP and head_here == 1 and key_dim == LANES and val_dim == LANES
    out_cols = out_weight.shape[1]
    flipped = fw % LANES == 0
    slots = LANES // (1 << level_total.bit_length())
    owned, out_rows, groups = seqs // levels, seqs // heads, seqs // GROUP
    f32, bf16 = jnp.float32, jnp.bfloat16
    vmem, anyspace = pl.BlockSpec(memory_space=pltpu.VMEM), pl.BlockSpec(memory_space=pl.ANY)
    dma = pltpu.SemaphoreType.DMA
    return pl.pallas_call(
        functools.partial(kernel, heads, levels, in_gain.shape[0], (key_dim, val_dim, level_total, level_here)),
        out_shape=pltpu.VMEM((out_rows, out_cols), f32),
        in_specs=[anyspace] * 8,
        out_specs=vmem,
        scratch_shapes=[
            pltpu.VMEM((heads * levels, fw), f32),
            pltpu.VMEM(level_bias.shape, f32),
            pltpu.VMEM((1, seqs), jnp.int32),
            pltpu.VMEM((1, val_dim), f32),
            pltpu.VMEM((heads, seqs, fw), f32),
            pltpu.VMEM((cols, width) if flipped else (width, cols), bf16),
            pltpu.VMEM((seqs, level_here * key_dim, val_dim), bf16),
            pltpu.VMEM(out_weight.shape, bf16),
            pltpu.VMEM((seqs, LANES), f32),
            pltpu.VMEM((levels, seqs // slots, LANES), f32),
            pltpu.VMEM((levels, seqs, key_dim), f32),
            pltpu.VMEM((seqs, key_dim), f32),
            pltpu.VMEM((levels, heads, owned, fw), f32),
            pltpu.VMEM((seqs, val_dim), f32),
            pltpu.VMEM((owned, 3 * LANES), f32),
            pltpu.VMEM((owned, fw), f32),
            pltpu.VMEM((owned, val_dim), f32),
            pltpu.VMEM((seqs, level_here * key_dim), f32),
            pltpu.VMEM((seqs, 2 * LANES), f32),
            pltpu.VMEM((levels, seqs, val_dim), f32),
            pltpu.VMEM((groups, heads // groups, out_rows, out_cols), f32),
            pltpu.VMEM((heads, out_rows, out_cols), f32),
            pltpu.VMEM((groups, 1, LANES), f32),
            pltpu.VMEM((heads, 1, LANES), f32),
            pltpu.VMEM((1, LANES), f32),
            pltpu.SemaphoreType.REGULAR,
            *[dma(())] * 5, dma((heads,)), dma(()), dma(()),
            dma(()), dma((groups,)), dma((levels,)), dma((groups,)), dma(()), dma(()),
        ],
        compiler_params=pltpu.CompilerParams(collective_id=0, has_side_effects=True),
    )(
        features,
        in_gain.reshape(heads * levels, fw),
        in_weight.T if flipped else in_weight,
        level_bias,
        states.reshape(seqs, level_here * key_dim, val_dim),
        positions.reshape(1, seqs),
        out_gain.reshape(1, val_dim),
        out_weight,
    )


def solution(mesh):
    in_specs = (
        P(None, ("head", "level")),
        P(),
        P(None, "head"),
        P("head", None),
        P(None, "head", "level", None, None),
        P(),
        P("head"),
        P("head", "level"),
    )
    out_specs = P("head", "level")
    return jax.shard_map(body, mesh=mesh, in_specs=in_specs, out_specs=out_specs, check_vma=False)
```
